128 devices in a mesh: head: 8 (over y, z_lo), ctx: 16 (over z_hi, x, core).
Axes of the slice: x: 4, y: 4, z: 4 (z_hi: 2, z_lo: 2; z = z_hi * 2 + z_lo), core: 2. Of those that a mesh axis runs over, the one named last changes fastest.
Arguments:
- query: bfloat16 [12288, 4096], P(('ctx', 'head')), may hold values from -8 to 8
- key: bfloat16 [12288, 2048], P(('ctx', 'head')), may hold values from -8 to 8
- value: bfloat16 [12288, 2048], P(('ctx', 'head')), may hold values from -8 to 8
- block_order: int32 [32], replicated, may hold values from 0 to 31, each once
Outputs:
- attended: bfloat16 [12288, 4096], P('ctx', 'head')
The draws below stay inside these ranges and needn't reach their ends.
Inputs may be any that keep to these rules, and one draw needn't show every extreme that they name: `block_order`: each storage block index 0 to 31 appears exactly once.
All inputs are finite; a program needn't handle non-finite values.
Results may differ from the reference program's by a relative error of at most 0.0049.
Values may be sent and summed in bfloat16 or wider, within the bound.
No kernel may reach another device: no remote copies, remote signals or barrier semaphores. Data moves between devices by JAX's collectives and lax.ppermute only.
A program may use at most 128 MiB of HBM per device.

```python
import jax
import jax.numpy as jnp
from jax import lax

HQ = 32
KEY_HEADS = 16
HEAD_WIDTH = 128
QUERY_PER_KEY = 2
TOKEN_COUNT = 12288
BLK = 384
BLOCKS = 32


def levels(stream_key, dims, split, low, high):
    factor_of, own = 1.0, jax.random.fold_in(stream_key, 6)
    for position, shards_of in split:
        draws = jnp.exp(jax.random.uniform(jax.random.fold_in(own, position), (shards_of,), jnp.float32, low / len(split), high / len(split)))
        factor_of = factor_of * jnp.repeat(draws, dims[position] // shards_of).reshape([-1 if axis == position else 1 for axis in range(len(dims))])
    return factor_of


def scatter_about(stream_key, shape, spread, most, cuts=(), held_as=jnp.bfloat16):
    values = spread * jax.random.normal(stream_key, shape, jnp.float32)
    if cuts:
        values = values * levels(stream_key, shape, cuts, -0.22, 0.18)
    return jnp.clip(values, -most, most).astype(held_as)


def setup_inputs(seed: int = 0) -> dict:
    streams_of = jax.random.split(jax.random.key(seed), 5)
    query = scatter_about(streams_of[0], (TOKEN_COUNT, HQ * HEAD_WIDTH), 1.5, 8.0, ((0, 128),))
    key = scatter_about(streams_of[1], (TOKEN_COUNT, KEY_HEADS * HEAD_WIDTH), 1.0, 8.0, ((0, 128),))
    value = scatter_about(streams_of[2], (TOKEN_COUNT, KEY_HEADS * HEAD_WIDTH), 1.0, 8.0, ((0, 128),))
    block_order = jax.random.permutation(streams_of[3], BLOCKS).astype(jnp.int32)
    return {"query": query, "key": key, "value": value, "block_order": block_order}


query_scale = 1.0 / 12.0
softcap_limit = 50.0


def head_block(query_rows, key_rows, value_rows, query_pos, key_pos):
    scores = jnp.einsum('rgd,kd->grk', query_rows.astype(jnp.float32), key_rows.astype(jnp.float32)) * query_scale
    capped = softcap_limit * jnp.tanh(scores / softcap_limit)
    visible = key_pos[None, :] <= query_pos[:, None]
    weights = jnp.where(visible[None], jnp.exp(capped), jnp.zeros_like(capped))
    denominator = jnp.sum(weights, axis=-1)
    rounded = lax.optimization_barrier(weights.astype(jnp.bfloat16)).astype(jnp.float32)
    numerator = jnp.einsum('grk,kd->grd', rounded, value_rows.astype(jnp.float32))
    return jnp.transpose(numerator / denominator[..., None], (1, 0, 2))


def reference(query, key, value, block_order):
    sequence_length = query.shape[0]
    positions = (block_order[:, None].astype(jnp.int32) * BLK + jnp.arange(BLK, dtype=jnp.int32)[None, :]).reshape(sequence_length)
    row_block = 2 * BLK
    block_count = sequence_length // row_block
    query_rows = query.reshape(sequence_length, KEY_HEADS, QUERY_PER_KEY, HEAD_WIDTH)
    key_rows = key.reshape(sequence_length, KEY_HEADS, HEAD_WIDTH)
    value_rows = value.reshape(sequence_length, KEY_HEADS, HEAD_WIDTH)
    columns = []
    for key_value_head in range(KEY_HEADS):
        def one_block(pieces, key_value_head=key_value_head):
            return head_block(pieces[0], key_rows[:, key_value_head], value_rows[:, key_value_head], pieces[1], positions)
        blocks = lax.map(one_block, (query_rows[:, key_value_head].reshape(block_count, row_block, QUERY_PER_KEY, HEAD_WIDTH), positions.reshape(block_count, row_block)))
        columns.append(blocks.reshape(sequence_length, QUERY_PER_KEY * HEAD_WIDTH))
    return jnp.concatenate(columns, axis=1).astype(jnp.bfloat16)
```

```python
import functools

import jax
import jax.numpy as jnp
from jax import lax
from jax.experimental import pallas as pl
from jax.experimental.pallas import tpu as pltpu
from jax.sharding import Mesh
from jax.sharding import PartitionSpec as P

HEAD = 128
BLK = 384
PIECE = 96
TILE = 256
Q_BLOCKS = 8
TILES = Q_BLOCKS * BLK // TILE
DUMMY = TILES
SCORE_SCALE = 1.0 / (12.0 * 50.0)
CAP_LOG2E = 50.0 * 1.4426950408889634

AXES = ("y", "zlo", "zhi", "x", "core")


def attend_kernel(*refs, offsets, first, last):
    n_shards = len(offsets)
    nb = 4 * n_shards
    refs = list(refs)
    order = refs.pop(0)
    kv = [refs.pop(0) for _ in range(n_shards)]
    if first:
        q_ref = refs.pop(0)
    else:
        qt_in, num_in, den_in = (refs.pop(0) for _ in range(3))
    if last:
        out_ref = refs.pop(0)
    else:
        qt_out, num_out, den_out = (refs.pop(0) for _ in range(3))
    qt, num, den, qpos, kbuf, vt, s0, s1, p0, p1, rows, q_seq, q_slot, kb_list, kb_start, kb_seq = refs

    x = lax.axis_index("x")
    core = lax.axis_index("core")

    seqs = []
    for slot in range(Q_BLOCKS):
        yhi, zhi, cc = slot // 4, (slot // 2) % 2, slot % 2
        seqs.append(order[2 * (zhi * 8 + x * 2 + cc) + yhi])
    for slot in range(Q_BLOCKS):
        rank = jnp.int32(0)
        for other in range(Q_BLOCKS):
            if other != slot:
                rank = rank + (seqs[other] < seqs[slot]).astype(jnp.int32)
        q_seq[rank] = seqs[slot]
        q_slot[rank] = jnp.int32(slot)

    lane = lax.broadcasted_iota(jnp.int32, (8, 128), 1)
    for g in range(2 * TILES):
        base = q_seq[g // 3] * BLK + (g % 3) * 128
        qpos[g // 2, :, (g % 2) * 128 : (g % 2) * 128 + 128] = lane + base

    if first:
        for rank in range(Q_BLOCKS):
            slot = q_slot[rank]
            yhi = slot // 4
            rest = slot % 4
            for sub in range(4):
                rows[pl.ds(rank * BLK + sub * PIECE, PIECE), :] = q_ref[yhi * 16 + sub * 4 + rest]
        for t in range(TILES):
            qt[t] = rows[t * TILE : (t + 1) * TILE, :].T
            num[t] = jnp.zeros((HEAD, TILE), jnp.float32)
            den[t] = jnp.zeros((8, TILE), jnp.float32)
    else:
        for t in range(TILES):
            qt[t] = qt_in[t]
            num[t] = num_in[t]
            den[t] = den_in[t]
    qt[DUMMY] = jnp.zeros((HEAD, TILE), jnp.bfloat16)
    num[DUMMY] = jnp.zeros((HEAD, TILE), jnp.float32)
    den[DUMMY] = jnp.zeros((8, TILE), jnp.float32)
    qpos[DUMMY] = jnp.zeros((8, TILE), jnp.int32)

    count = jnp.int32(0)
    total = jnp.int32(0)
    for n, (dx, flip) in enumerate(offsets):
        xs = (x + (4 - dx)) % 4
        cs = core + flip - 2 * core * flip
        for b in range(4):
            yhi, zhi = b // 2, b % 2
            kb = 4 * n + b
            vals = []
            for sub in range(4):
                piece = kv[n][yhi * 8 + sub * 2 + zhi]
                kbuf[kb, sub * PIECE : (sub + 1) * PIECE, :] = piece[:, :HEAD]
                vals.append(piece[:, HEAD:])
            vt[kb] = jnp.concatenate(vals, axis=0).T
            seq = order[2 * (zhi * 8 + xs * 2 + cs) + yhi]
            below = jnp.int32(0)
            for rank in range(Q_BLOCKS):
                below = below + (q_seq[rank] < seq).astype(jnp.int32)
            start = (3 * below) // 2
            kb_list[count] = jnp.int32(kb)
            kb_start[count] = start
            kb_seq[count] = seq
            has = (start < TILES).astype(jnp.int32)
            count = count + has
            total = total + (TILES - start)
    for extra in range(6):
        kb_list[count + extra] = jnp.int32(0)
        kb_start[count + extra] = jnp.int32(DUMMY)
        kb_seq[count + extra] = jnp.int32(0)

    def after(item):
        j, t = item
        wrap = t + 1 >= TILES
        j = jnp.where(wrap, j + 1, j)
        return j, jnp.where(wrap, kb_start[j], t + 1)

    def score(item, s):
        j, t = item
        s[...] = jnp.dot(kbuf[kb_list[j]], qt[t], preferred_element_type=jnp.float32)

    row = lax.broadcasted_iota(jnp.int32, (8, TILE), 0)

    def weigh(item, s, p):
        j, t = item
        rel = qpos[t] - kb_seq[j] * BLK
        acc = den[t]
        for r in range(0, BLK, 16):
            halves = []
            for h in range(2):
                z = s[r + 8 * h : r + 8 * h + 8, :]
                w = jnp.exp2(CAP_LOG2E * jnp.tanh(z * SCORE_SCALE))
                w = jnp.where(row + (r + 8 * h) <= rel, w, 0.0)
                acc = acc + w
                halves.append(w)
            p[r : r + 16, :] = jnp.concatenate(halves, axis=0).astype(jnp.bfloat16)
        den[t] = acc

    def gather(item, p):
        j, t = item
        num[t] = num[t] + jnp.dot(vt[kb_list[j]], p[...], preferred_element_type=jnp.float32)

    i0 = (jnp.int32(0), kb_start[0])
    i1 = after(i0)
    score(i0, s0)
    score(i1, s1)
    p0[...] = jnp.zeros_like(p0)
    p1[...] = jnp.zeros_like(p1)
    dummy = (count, jnp.int32(DUMMY))

    def body(_, state):
        a, b, pa, pb = state
        na = after(b)
        nb_ = after(na)
        gather(pa, p0)
        gather(pb, p1)
        weigh(a, s0, p0)
        weigh(b, s1, p1)
        score(na, s0)
        score(nb_, s1)
        return na, nb_, a, b

    _, _, pa, pb = lax.fori_loop(0, (total + 1) // 2, body, (i0, i1, dummy, dummy))
    gather(pa, p0)
    gather(pb, p1)

    if last:
        for t in range(TILES):
            inv = 1.0 / jnp.sum(den[t], axis=0, keepdims=True)
            rows[t * TILE : (t + 1) * TILE, :] = (num[t] * inv).T.astype(jnp.bfloat16)
        for rank in range(Q_BLOCKS):
            slot = q_slot[rank]
            yhi = slot // 4
            rest = slot % 4
            out_ref[rest, pl.ds(pl.multiple_of(yhi * BLK, BLK), BLK), :] = rows[
                rank * BLK : (rank + 1) * BLK, :
            ]
    else:
        for t in range(TILES):
            qt_out[t] = qt[t]
            num_out[t] = num[t]
            den_out[t] = den[t]


def attend(order, kvs, offsets, carry, first, last):
    vmem = pl.BlockSpec(memory_space=pltpu.VMEM)
    smem = pl.BlockSpec(memory_space=pltpu.SMEM)
    nb = 4 * len(kvs)
    state = (
        jax.ShapeDtypeStruct((TILES, HEAD, TILE), jnp.bfloat16),
        jax.ShapeDtypeStruct((TILES, HEAD, TILE), jnp.float32),
        jax.ShapeDtypeStruct((TILES, 8, TILE), jnp.float32),
    )
    if last:
        out = jax.ShapeDtypeStruct((4, 2 * BLK, HEAD), jnp.bfloat16)
        out_specs = vmem
    else:
        out = state
        out_specs = (vmem, vmem, vmem)
    inputs = [order, *kvs, *carry]
    return pl.pallas_call(
        functools.partial(attend_kernel, offsets=offsets, first=first, last=last),
        out_shape=out,
        in_specs=[smem] + [vmem] * (len(inputs) - 1),
        out_specs=out_specs,
        scratch_shapes=[
            pltpu.VMEM((TILES + 1, HEAD, TILE), jnp.bfloat16),
            pltpu.VMEM((TILES + 1, HEAD, TILE), jnp.float32),
            pltpu.VMEM((TILES + 1, 8, TILE), jnp.float32),
            pltpu.VMEM((TILES + 1, 8, TILE), jnp.int32),
            pltpu.VMEM((nb, BLK, HEAD), jnp.bfloat16),
            pltpu.VMEM((nb, HEAD, BLK), jnp.bfloat16),
            pltpu.VMEM((BLK, TILE), jnp.float32),
            pltpu.VMEM((BLK, TILE), jnp.float32),
            pltpu.VMEM((BLK, TILE), jnp.bfloat16),
            pltpu.VMEM((BLK, TILE), jnp.bfloat16),
            pltpu.VMEM((Q_BLOCKS * BLK, HEAD), jnp.bfloat16),
            pltpu.SMEM((Q_BLOCKS,), jnp.int32),
            pltpu.SMEM((Q_BLOCKS,), jnp.int32),
            pltpu.SMEM((nb + 8,), jnp.int32),
            pltpu.SMEM((nb + 8,), jnp.int32),
            pltpu.SMEM((nb + 8,), jnp.int32),
        ],
        compiler_params=pltpu.CompilerParams(vmem_limit_bytes=40 * 1024 * 1024),
        cost_estimate=pl.CostEstimate(
            flops=len(kvs) * 2_400_000_000, transcendentals=0, bytes_accessed=4_000_000
        ),
        name=f"attend_{len(kvs)}_{int(first)}{int(last)}",
    )(*inputs)


def along_x(value, by):
    return lax.ppermute(value, "x", [(i, (i + by) % 4) for i in range(4)])


def other_core(value):
    return lax.ppermute(value, "core", [(0, 1), (1, 0)])


def shards(query, key, value, block_order):
    rows = query.shape[0]
    kv = jnp.concatenate(
        [key.reshape(rows, 16, HEAD), value.reshape(rows, 16, HEAD)], axis=2
    ).transpose(1, 0, 2)
    kv = lax.all_to_all(kv, ("y", "zlo", "zhi"), 0, 0)
    q = query.reshape(rows, 32, HEAD).transpose(1, 0, 2)
    q = lax.all_to_all(q, ("y", "zlo", "zhi", "core"), 0, 0)

    own_other = other_core(kv)
    up = along_x(kv, 1)
    down = along_x(kv, -1)
    far_a = along_x(up[:8], 1)
    far_b = along_x(down[8:], -1)
    up_other = other_core(up)
    down_other = other_core(down)
    far = jnp.concatenate([far_a, far_b], axis=0)
    far_other = other_core(far)

    state = attend(block_order, (kv, own_other), ((0, 0), (0, 1)), (q,), True, False)
    state = attend(
        block_order,
        (up, down, up_other, down_other),
        ((1, 0), (3, 0), (1, 1), (3, 1)),
        state,
        False,
        False,
    )
    out = attend(block_order, (far, far_other), ((2, 0), (2, 1)), state, False, True)
    out = lax.all_to_all(out, ("zhi", "core"), 0, 0)
    return out.transpose(1, 0, 2).reshape(2 * BLK, 4 * HEAD)


def solution(mesh):
    fine = Mesh(mesh.devices.reshape(4, 2, 2, 4, 2), AXES)
    placed = P(("zhi", "x", "core", "y", "zlo"), None)
    return jax.shard_map(
        shards,
        mesh=fine,
        in_specs=(placed, placed, placed, P()),
        out_specs=P(("zhi", "x", "core"), ("y", "zlo")),
        check_vma=False,
    )
```

```python
import functools

import jax
import jax.numpy as jnp
from jax import lax
from jax.experimental import pallas as pl
from jax.experimental.pallas import tpu as pltpu
from jax.sharding import Mesh
from jax.sharding import PartitionSpec as P

HEAD = 128
BLK = 384
PIECE = 96
TILE = 256
HALF_BLOCKS = 4
TILES = HALF_BLOCKS * BLK // TILE
UNROLL = 4
SCORE_SCALE = 1.0 / (12.0 * 50.0)
CAP_LOG2E = 50.0 * 1.4426950408889634

AXES = ("y", "zlo", "zhi", "x", "core")
REMOTE, LOCAL = 0, 1


def attend_kernel(*refs, offsets, halves, first, last):
    n_halves = len(halves)
    dummy_tile = n_halves * TILES
    refs = list(refs)
    order = refs.pop(0)
    kv = []
    for _, _, parts in offsets:
        pieces = [refs.pop(0) for _ in range(parts)]
        kv.append([(pieces[0], 0), (pieces[-1], 0 if parts == 2 else 8)])
    if first:
        q_ref = refs.pop(0)
    else:
        states_in = [[refs.pop(0) for _ in range(3)] for _ in halves]
    if last:
        outs = [[refs.pop(0) for _ in range(2)] for _ in halves]
    else:
        states_out = [[refs.pop(0) for _ in range(3)] for _ in halves]
    qt, num, den, qpos, kbuf, vt = refs[:6]
    s_bufs = refs[6 : 6 + UNROLL]
    p_bufs = refs[6 + UNROLL : 6 + 2 * UNROLL]
    rows, q_seq, q_rank, kb_list, kb_start, kb_end, kb_seq = refs[6 + 2 * UNROLL :]

    x = lax.axis_index("x")
    core = lax.axis_index("core")
    zhi = lax.axis_index("zhi")

    lane = lax.broadcasted_iota(jnp.int32, (8, 128), 1)
    where_from = []
    for n, half in enumerate(halves):
        zz = 1 - zhi if half == REMOTE else zhi
        seqs = []
        for slot in range(HALF_BLOCKS):
            yhi, flip = slot // 2, slot % 2
            cc = 1 - core if flip else core
            where_from.append(yhi * 16 + zz * 2 + cc)
            seqs.append(order[2 * (zz * 8 + x * 2 + cc) + yhi])
        for slot in range(HALF_BLOCKS):
            rank = jnp.int32(4 * n)
            for other in range(HALF_BLOCKS):
                if other != slot:
                    rank = rank + (seqs[other] < seqs[slot]).astype(jnp.int32)
            q_seq[rank] = seqs[slot]
            q_rank[4 * n + slot] = rank
    for g in range(2 * n_halves * TILES):
        base = q_seq[g // 3] * BLK + (g % 3) * 128
        qpos[g // 2, :, (g % 2) * 128 : (g % 2) * 128 + 128] = lane + base
    qpos[dummy_tile] = jnp.zeros((8, TILE), jnp.int32)

    if first:
        for slot in range(HALF_BLOCKS * n_halves):
            top = pl.multiple_of(q_rank[slot] * BLK, BLK)
            for sub in range(4):
                rows[pl.ds(top + sub * PIECE, PIECE), :] = q_ref[where_from[slot] + sub * 4]
        for t in range(n_halves * TILES):
            qt[t] = rows[t * TILE : (t + 1) * TILE, :].T
            num[t] = jnp.zeros((HEAD, TILE), jnp.float32)
            den[t] = jnp.zeros((8, TILE), jnp.float32)
    else:
        for n in range(n_halves):
            for t in range(TILES):
                qt[n * TILES + t] = states_in[n][0][t]
                num[n * TILES + t] = states_in[n][1][t]
                den[n * TILES + t] = states_in[n][2][t]
    qt[dummy_tile] = jnp.zeros((HEAD, TILE), jnp.bfloat16)
    num[dummy_tile] = jnp.zeros((HEAD, TILE), jnp.float32)
    den[dummy_tile] = jnp.zeros((8, TILE), jnp.float32)

    count = jnp.int32(0)
    total = jnp.int32(0)
    for n, (dx, flip, _) in enumerate(offsets):
        xs = (x + (4 - dx)) % 4
        cs = 1 - core if flip else core
        for b in range(4):
            yhi, zz = b // 2, b % 2
            kb = 4 * n + b
            vals = []
            for sub in range(4):
                source, at = kv[n][yhi]
                piece = source[at + sub * 2 + zz]
                kbuf[kb, sub * PIECE : (sub + 1) * PIECE, :] = piece[:, :HEAD]
                vals.append(piece[:, HEAD:])
            vt[kb] = jnp.concatenate(vals, axis=0).T
            seq = order[2 * (zz * 8 + xs * 2 + cs) + yhi]
            for h in range(n_halves):
                below = jnp.int32(0)
                for rank in range(HALF_BLOCKS):
                    below = below + (q_seq[4 * h + rank] < seq).astype(jnp.int32)
                start = (3 * below) // 2
                kb_list[count] = jnp.int32(kb)
                kb_start[count] = start + h * TILES
                kb_end[count] = jnp.int32((h + 1) * TILES)
                kb_seq[count] = seq
                count = count + (start < TILES).astype(jnp.int32)
                total = total + (TILES - start)
    for extra in range(2 * UNROLL + 2):
        kb_list[count + extra] = jnp.int32(0)
        kb_start[count + extra] = jnp.int32(dummy_tile)
        kb_end[count + extra] = jnp.int32(0)
        kb_seq[count + extra] = jnp.int32(0)

    def after(item):
        j, t = item
        wrap = t + 1 >= kb_end[j]
        j = jnp.where(wrap, j + 1, j)
        return j, jnp.where(wrap, kb_start[j], t + 1)

    def score(item, s):
        j, t = item
        s[...] = jnp.dot(kbuf[kb_list[j]], qt[t], preferred_element_type=jnp.float32)

    row = lax.broadcasted_iota(jnp.int32, (8, TILE), 0)

    def weigh(item, s, p):
        j, t = item
        rel = qpos[t] - kb_seq[j] * BLK
        acc = None
        for r in range(0, BLK, 16):
            both = []
            for h in range(2):
                z = s[r + 8 * h : r + 8 * h + 8, :]
                w = jnp.exp2(CAP_LOG2E * jnp.tanh(z * SCORE_SCALE))
                w = jnp.where(row + (r + 8 * h) <= rel, w, 0.0)
                acc = w if acc is None else acc + w
                both.append(w)
            p[r : r + 16, :] = jnp.concatenate(both, axis=0).astype(jnp.bfloat16)
        den[t] = den[t] + acc

    def gather(item, p):
        j, t = item
        num[t] = num[t] + jnp.dot(vt[kb_list[j]], p[...], preferred_element_type=jnp.float32)

    items = [(jnp.int32(0), kb_start[0])]
    for _ in range(UNROLL - 1):
        items.append(after(items[-1]))
    for k in range(UNROLL):
        score(items[k], s_bufs[k])
    p_bufs[UNROLL - 1][...] = jnp.zeros((BLK, TILE), jnp.bfloat16)

    def body(_, state):
        cur, prev = state
        nxt = []
        item = cur[-1]
        for _ in range(UNROLL):
            item = after(item)
            nxt.append(item)
        for k in range(UNROLL):
            weigh(cur[k], s_bufs[k], p_bufs[k])
            score(nxt[k], s_bufs[k])
            if k == 0:
                gather(prev, p_bufs[UNROLL - 1])
            else:
                gather(cur[k - 1], p_bufs[k - 1])
        return tuple(nxt), cur[-1]

    idle = (count, jnp.int32(dummy_tile))
    _, tail = lax.fori_loop(0, (total + UNROLL - 1) // UNROLL, body, (tuple(items), idle))
    gather(tail, p_bufs[UNROLL - 1])

    if last:
        for t in range(n_halves * TILES):
            inv = 1.0 / jnp.sum(den[t], axis=0, keepdims=True)
            rows[t * TILE : (t + 1) * TILE, :] = (num[t] * inv).T.astype(jnp.bfloat16)
        for n in range(n_halves):
            for slot in range(HALF_BLOCKS):
                yhi, flip = slot // 2, slot % 2
                top = pl.multiple_of(q_rank[4 * n + slot] * BLK, BLK)
                outs[n][flip][yhi * BLK : (yhi + 1) * BLK, :] = rows[pl.ds(top, BLK), :]
    else:
        for n in range(n_halves):
            for t in range(TILES):
                states_out[n][0][t] = qt[n * TILES + t]
                states_out[n][1][t] = num[n * TILES + t]
                states_out[n][2][t] = den[n * TILES + t]


def attend(order, given, halves, carry, first, last):
    kvs = [piece for pieces, _, _ in given for piece in pieces]
    offsets = tuple((dx, flip, len(pieces)) for pieces, dx, flip in given)
    vmem = pl.BlockSpec(memory_space=pltpu.VMEM)
    smem = pl.BlockSpec(memory_space=pltpu.SMEM)
    nb = 4 * len(given)
    tiles = TILES * len(halves)
    runs = nb * len(halves) + 2 * UNROLL + 4
    if last:
        out = (jax.ShapeDtypeStruct((2 * BLK, HEAD), jnp.bfloat16),) * (2 * len(halves))
    else:
        out = (
            jax.ShapeDtypeStruct((TILES, HEAD, TILE), jnp.bfloat16),
            jax.ShapeDtypeStruct((TILES, HEAD, TILE), jnp.float32),
            jax.ShapeDtypeStruct((TILES, 8, TILE), jnp.float32),
        ) * len(halves)
    inputs = [order, *kvs, *carry]
    return pl.pallas_call(
        functools.partial(attend_kernel, offsets=offsets, halves=halves, first=first, last=last),
        out_shape=out,
        in_specs=[smem] + [vmem] * (len(inputs) - 1),
        out_specs=(vmem,) * len(out),
        scratch_shapes=[
            pltpu.VMEM((tiles + 1, HEAD, TILE), jnp.bfloat16),
            pltpu.VMEM((tiles + 1, HEAD, TILE), jnp.float32),
            pltpu.VMEM((tiles + 1, 8, TILE), jnp.float32),
            pltpu.VMEM((tiles + 1, 8, TILE), jnp.int32),
            pltpu.VMEM((nb, BLK, HEAD), jnp.bfloat16),
            pltpu.VMEM((nb, HEAD, BLK), jnp.bfloat16),
            *[pltpu.VMEM((BLK, TILE), jnp.float32) for _ in range(UNROLL)],
            *[pltpu.VMEM((BLK, TILE), jnp.bfloat16) for _ in range(UNROLL)],
            pltpu.VMEM((tiles * TILE, HEAD), jnp.bfloat16),
            pltpu.SMEM((HALF_BLOCKS * len(halves),), jnp.int32),
            pltpu.SMEM((HALF_BLOCKS * len(halves),), jnp.int32),
            pltpu.SMEM((runs,), jnp.int32),
            pltpu.SMEM((runs,), jnp.int32),
            pltpu.SMEM((runs,), jnp.int32),
            pltpu.SMEM((runs,), jnp.int32),
        ],
        compiler_params=pltpu.CompilerParams(vmem_limit_bytes=36 * 1024 * 1024),
        cost_estimate=pl.CostEstimate(
            flops=len(given) * len(halves) * 1_200_000_000,
            transcendentals=0,
            bytes_accessed=4_000_000,
        ),
    )(*inputs)


def assemble_kernel(own, swapped, z_same, z_cross, out):
    zhi = lax.axis_index("zhi")
    core = lax.axis_index("core")
    for piece, zz, cc in (
        (z_same, 1 - zhi, core),
        (z_cross, 1 - zhi, 1 - core),
        (own, zhi, core),
        (swapped, zhi, 1 - core),
    ):
        left = pl.multiple_of((zz * 2 + cc) * HEAD, HEAD)
        out[:, pl.ds(left, HEAD)] = piece[...]


def along_x(value, by):
    return lax.ppermute(value, "x", [(i, (i + by) % 4) for i in range(4)])


def other_core(value):
    return lax.ppermute(value, "core", [(0, 1), (1, 0)])


def layer(query, key, value, block_order):
    rows = query.shape[0]
    kv = jnp.concatenate(
        [key.reshape(rows, 16, HEAD), value.reshape(rows, 16, HEAD)], axis=2
    ).transpose(1, 0, 2)
    kv = lax.all_to_all(kv, ("y", "zlo", "zhi"), 0, 0)
    q = query.reshape(rows, 32, HEAD).transpose(1, 0, 2)
    q = lax.all_to_all(q, ("y", "zlo", "zhi", "core"), 0, 0)

    up = along_x(kv, 1)
    down = along_x(kv, -1)
    own_o = other_core(kv)
    far_a = along_x(up[:8], 1)
    far_b = along_x(down[8:], -1)
    up_o = other_core(up)
    down_o = other_core(down)
    far_a_o = other_core(far_a)
    far_b_o = other_core(far_b)

    near = [((up,), 1, 0), ((down,), 3, 0)]
    near_o = [((up_o,), 1, 1), ((down_o,), 3, 1)]
    far = [((far_a, far_b), 2, 0), ((far_a_o, far_b_o), 2, 1)]

    def step(given, halves, carry, first=False, last=False):
        return attend(block_order, given, halves, carry, first, last)

    state = step([((kv,), 0, 0)], (REMOTE, LOCAL), (q,), first=True)
    state = step([((own_o,), 0, 1)], (REMOTE, LOCAL), state)
    remote, local = state[:3], state[3:]
    remote = step(near, (REMOTE,), remote)
    remote = step(near_o, (REMOTE,), remote)
    same, cross = step(far, (REMOTE,), remote, last=True)
    z_same = lax.ppermute(same, "zhi", [(0, 1), (1, 0)])
    z_cross = lax.ppermute(cross, ("zhi", "core"), [(i, 3 - i) for i in range(4)])
    own, cross = step(near + near_o + far, (LOCAL,), local, last=True)
    swapped = other_core(cross)
    vmem = pl.BlockSpec(memory_space=pltpu.VMEM)
    return pl.pallas_call(
        assemble_kernel,
        out_shape=jax.ShapeDtypeStruct((2 * BLK, 4 * HEAD), jnp.bfloat16),
        in_specs=[vmem] * 4,
        out_specs=vmem,
        name="assemble",
    )(own, swapped, z_same, z_cross)


def solution(mesh):
    fine = Mesh(mesh.devices.reshape(4, 2, 2, 4, 2), AXES)
    placed = P(("zhi", "x", "core", "y", "zlo"), None)
    return jax.shard_map(
        layer,
        mesh=fine,
        in_specs=(placed, placed, placed, P()),
        out_specs=P(("zhi", "x", "core"), ("y", "zlo")),
        check_vma=False,
    )
```

```python
import functools

import jax
import jax.numpy as jnp
from jax import lax
from jax.experimental import pallas as pl
from jax.experimental.pallas import tpu as pltpu
from jax.sharding import Mesh
from jax.sharding import PartitionSpec as P

HEAD = 128
BLK = 384
PIECE = 96
TILE = 256
HALF_BLOCKS = 4
TILES = HALF_BLOCKS * BLK // TILE
UNROLL = 4
SCORE_SCALE = 1.0 / (12.0 * 50.0)
CAP_LOG2E = 50.0 * 1.4426950408889634

AXES = ("y", "zlo", "zhi", "x", "core")
REMOTE, LOCAL = 0, 1


def attend_kernel(*refs, offsets, halves, first, last):
    n_shards = len(offsets)
    n_halves = len(halves)
    dummy_tile = n_halves * TILES
    refs = list(refs)
    order = refs.pop(0)
    kv = [[refs.pop(0) for _ in range(2)] for _ in range(n_shards)]
    if first:
        q_refs = [refs.pop(0) for _ in range(4)]
    else:
        states_in = [[refs.pop(0) for _ in range(3)] for _ in halves]
    if last:
        outs = [[refs.pop(0) for _ in range(2)] for _ in halves]
    else:
        states_out = [[refs.pop(0) for _ in range(3)] for _ in halves]
    qt, num, den, qpos, kbuf, vbuf, vt = refs[:7]
    s_bufs = refs[7 : 7 + UNROLL]
    p_bufs = refs[7 + UNROLL : 7 + 2 * UNROLL]
    rows, q_seq, q_rank, kb_list, kb_start, kb_end, kb_seq = refs[7 + 2 * UNROLL :]

    x = lax.axis_index("x")
    core = lax.axis_index("core")
    zhi = lax.axis_index("zhi")
    zlo = lax.axis_index("zlo")
    y = lax.axis_index("y")

    def sender(dy, e):
        ys = (y + (4 - dy)) % 4
        zl = 1 - zlo if e % 2 else zlo
        zh = 1 - zhi if e // 2 else zhi
        return ys // 2, pl.multiple_of(((ys % 2) * 2 + zl) * PIECE, PIECE), zh

    lane = lax.broadcasted_iota(jnp.int32, (8, 128), 1)
    for n, half in enumerate(halves):
        zz = 1 - zhi if half == REMOTE else zhi
        seqs = []
        for slot in range(HALF_BLOCKS):
            yhi, flip = slot // 2, slot % 2
            cc = 1 - core if flip else core
            seqs.append(order[2 * (zz * 8 + x * 2 + cc) + yhi])
        for slot in range(HALF_BLOCKS):
            rank = jnp.int32(4 * n)
            for other in range(HALF_BLOCKS):
                if other != slot:
                    rank = rank + (seqs[other] < seqs[slot]).astype(jnp.int32)
            q_seq[rank] = seqs[slot]
            q_rank[4 * n + slot] = rank
    for g in range(2 * n_halves * TILES):
        base = q_seq[g // 3] * BLK + (g % 3) * 128
        qpos[g // 2, :, (g % 2) * 128 : (g % 2) * 128 + 128] = lane + base
    qpos[dummy_tile] = jnp.zeros((8, TILE), jnp.int32)

    if first:
        for dy in range(4):
            for e in range(4):
                yhi, sub, _ = sender(dy, e)
                n = halves.index(REMOTE if e // 2 else LOCAL)
                for flip in range(2):
                    top = q_rank[4 * n + yhi * 2 + flip] * BLK + sub
                    rows[pl.ds(pl.multiple_of(top, PIECE), PIECE), :] = q_refs[dy][e, flip]
        for t in range(n_halves * TILES):
            qt[t] = rows[t * TILE : (t + 1) * TILE, :].T
            num[t] = jnp.zeros((HEAD, TILE), jnp.float32)
            den[t] = jnp.zeros((8, TILE), jnp.float32)
    else:
        for n in range(n_halves):
            for t in range(TILES):
                qt[n * TILES + t] = states_in[n][0][t]
                num[n * TILES + t] = states_in[n][1][t]
                den[n * TILES + t] = states_in[n][2][t]
    qt[dummy_tile] = jnp.zeros((HEAD, TILE), jnp.bfloat16)
    num[dummy_tile] = jnp.zeros((HEAD, TILE), jnp.float32)
    den[dummy_tile] = jnp.zeros((8, TILE), jnp.float32)

    count = jnp.int32(0)
    total = jnp.int32(0)
    for n, (dx, flip) in enumerate(offsets):
        for dy in range(4):
            for e in range(4):
                yhi, sub, zh = sender(dy, e)
                kb = 4 * n + yhi * 2 + zh
                piece = kv[n][dy // 2][dy % 2, e]
                kbuf[kb, pl.ds(sub, PIECE), :] = piece[:, :HEAD]
                vbuf[kb, pl.ds(sub, PIECE), :] = piece[:, HEAD:]
        xs = (x + (4 - dx)) % 4
        cs = 1 - core if flip else core
        for b in range(4):
            yhi, zz = b // 2, b % 2
            kb = 4 * n + b
            vt[kb] = vbuf[kb].T
            seq = order[2 * (zz * 8 + xs * 2 + cs) + yhi]
            for h in range(n_halves):
                below = jnp.int32(0)
                for rank in range(HALF_BLOCKS):
                    below = below + (q_seq[4 * h + rank] < seq).astype(jnp.int32)
                start = (3 * below) // 2
                kb_list[count] = jnp.int32(kb)
                kb_start[count] = start + h * TILES
                kb_end[count] = jnp.int32((h + 1) * TILES)
                kb_seq[count] = seq
                count = count + (start < TILES).astype(jnp.int32)
                total = total + (TILES - start)
    for extra in range(2 * UNROLL + 2):
        kb_list[count + extra] = jnp.int32(0)
        kb_start[count + extra] = jnp.int32(dummy_tile)
        kb_end[count + extra] = jnp.int32(0)
        kb_seq[count + extra] = jnp.int32(0)

    def after(item):
        j, t = item
        wrap = t + 1 >= kb_end[j]
        j = jnp.where(wrap, j + 1, j)
        return j, jnp.where(wrap, kb_start[j], t + 1)

    def score(item, s):
        j, t = item
        s[...] = jnp.dot(kbuf[kb_list[j]], qt[t], preferred_element_type=jnp.float32)

    row = lax.broadcasted_iota(jnp.int32, (8, TILE), 0)

    def weigh(item, s, p):
        j, t = item
        rel = qpos[t] - (kb_seq[j] * BLK + row)
        acc = None
        for r in range(0, BLK, 16):
            both = []
            for h in range(2):
                z = s[r + 8 * h : r + 8 * h + 8, :]
                w = jnp.exp2(CAP_LOG2E * jnp.tanh(z * SCORE_SCALE))
                w = jnp.where(rel >= r + 8 * h, w, 0.0)
                acc = w if acc is None else acc + w
                both.append(w)
            p[r : r + 16, :] = jnp.concatenate(both, axis=0).astype(jnp.bfloat16)
        den[t] = den[t] + acc

    def gather(item, p):
        j, t = item
        num[t] = num[t] + jnp.dot(vt[kb_list[j]], p[...], preferred_element_type=jnp.float32)

    items = [(jnp.int32(0), kb_start[0])]
    for _ in range(UNROLL - 1):
        items.append(after(items[-1]))
    for k in range(UNROLL):
        score(items[k], s_bufs[k])
    p_bufs[UNROLL - 1][...] = jnp.zeros((BLK, TILE), jnp.bfloat16)

    def body(_, state):
        cur, prev = state
        nxt = []
        item = cur[-1]
        for _ in range(UNROLL):
            item = after(item)
            nxt.append(item)
        for k in range(UNROLL):
            weigh(cur[k], s_bufs[k], p_bufs[k])
            score(nxt[k], s_bufs[k])
            if k == 0:
                gather(prev, p_bufs[UNROLL - 1])
            else:
                gather(cur[k - 1], p_bufs[k - 1])
        return tuple(nxt), cur[-1]

    idle = (count, jnp.int32(dummy_tile))
    _, tail = lax.fori_loop(0, (total + UNROLL - 1) // UNROLL, body, (tuple(items), idle))
    gather(tail, p_bufs[UNROLL - 1])

    if last:
        for t in range(n_halves * TILES):
            inv = 1.0 / jnp.sum(den[t], axis=0, keepdims=True)
            rows[t * TILE : (t + 1) * TILE, :] = (num[t] * inv).T.astype(jnp.bfloat16)
        for n in range(n_halves):
            for slot in range(HALF_BLOCKS):
                yhi, flip = slot // 2, slot % 2
                top = pl.multiple_of(q_rank[4 * n + slot] * BLK, BLK)
                outs[n][flip][yhi * BLK : (yhi + 1) * BLK, :] = rows[pl.ds(top, BLK), :]
    else:
        for n in range(n_halves):
            for t in range(TILES):
                states_out[n][0][t] = qt[n * TILES + t]
                states_out[n][1][t] = num[n * TILES + t]
                states_out[n][2][t] = den[n * TILES + t]


def attend(order, given, halves, carry, first, last):
    kvs = [piece for pieces, _, _ in given for piece in pieces]
    offsets = tuple((dx, flip) for _, dx, flip in given)
    vmem = pl.BlockSpec(memory_space=pltpu.VMEM)
    smem = pl.BlockSpec(memory_space=pltpu.SMEM)
    nb = 4 * len(given)
    tiles = TILES * len(halves)
    runs = nb * len(halves) + 2 * UNROLL + 4
    if last:
        out = (jax.ShapeDtypeStruct((2 * BLK, HEAD), jnp.bfloat16),) * (2 * len(halves))
    else:
        out = (
            jax.ShapeDtypeStruct((TILES, HEAD, TILE), jnp.bfloat16),
            jax.ShapeDtypeStruct((TILES, HEAD, TILE), jnp.float32),
            jax.ShapeDtypeStruct((TILES, 8, TILE), jnp.float32),
        ) * len(halves)
    inputs = [order, *kvs, *carry]
    return pl.pallas_call(
        functools.partial(attend_kernel, offsets=offsets, halves=halves, first=first, last=last),
        out_shape=out,
        in_specs=[smem] + [vmem] * (len(inputs) - 1),
        out_specs=(vmem,) * len(out),
        scratch_shapes=[
            pltpu.VMEM((tiles + 1, HEAD, TILE), jnp.bfloat16),
            pltpu.VMEM((tiles + 1, HEAD, TILE), jnp.float32),
            pltpu.VMEM((tiles + 1, 8, TILE), jnp.float32),
            pltpu.VMEM((tiles + 1, 8, TILE), jnp.int32),
            pltpu.VMEM((nb, BLK, HEAD), jnp.bfloat16),
            pltpu.VMEM((nb, BLK, HEAD), jnp.bfloat16),
            pltpu.VMEM((nb, HEAD, BLK), jnp.bfloat16),
            *[pltpu.VMEM((BLK, TILE), jnp.float32) for _ in range(UNROLL)],
            *[pltpu.VMEM((BLK, TILE), jnp.bfloat16) for _ in range(UNROLL)],
            pltpu.VMEM((tiles * TILE, HEAD), jnp.bfloat16),
            pltpu.SMEM((HALF_BLOCKS * len(halves),), jnp.int32),
            pltpu.SMEM((HALF_BLOCKS * len(halves),), jnp.int32),
            pltpu.SMEM((runs,), jnp.int32),
            pltpu.SMEM((runs,), jnp.int32),
            pltpu.SMEM((runs,), jnp.int32),
            pltpu.SMEM((runs,), jnp.int32),
        ],
        compiler_params=pltpu.CompilerParams(vmem_limit_bytes=36 * 1024 * 1024),
        cost_estimate=pl.CostEstimate(
            flops=len(given) * len(halves) * 1_200_000_000,
            transcendentals=0,
            bytes_accessed=4_000_000,
        ),
    )(*inputs)


def local_call(body, outs, inputs):
    vmem = pl.BlockSpec(memory_space=pltpu.VMEM)
    return pl.pallas_call(
        body,
        out_shape=tuple(jax.ShapeDtypeStruct(shape, jnp.bfloat16) for shape in outs),
        in_specs=[vmem] * len(inputs),
        out_specs=(vmem,) * len(outs),
        compiler_params=pltpu.CompilerParams(vmem_limit_bytes=8 * 1024 * 1024),
    )(*inputs)


def sort_kernel(query, key, value, kv0, kv1, kv2, kv3, keep, send):
    y, zlo, zhi = lax.axis_index("y"), lax.axis_index("zlo"), lax.axis_index("zhi")
    core = lax.axis_index("core")
    for e, out in enumerate((kv0, kv1, kv2, kv3)):
        zl = 1 - zlo if e % 2 else zlo
        zh = 1 - zhi if e // 2 else zhi
        for dy in range(4):
            head = (((y + dy) % 4) * 2 + zl) * 2 + zh
            at = pl.ds(pl.multiple_of(head * HEAD, HEAD), HEAD)
            out[dy, :, :HEAD] = key[:, at]
            out[dy, :, HEAD:] = value[:, at]
            mine = pl.multiple_of((2 * head + core) * HEAD, HEAD)
            other = pl.multiple_of((2 * head + 1 - core) * HEAD, HEAD)
            keep[e, dy] = query[:, pl.ds(mine, HEAD)]
            send[e, dy] = query[:, pl.ds(other, HEAD)]


def join_kernel(keep, got, q0, q1, q2, q3):
    for e, out in enumerate((q0, q1, q2, q3)):
        for dy in range(4):
            out[dy, 0] = keep[e, dy]
            out[dy, 1] = got[e, dy]


def turn_kernel(*refs):
    for dy in range(4):
        for e in range(4):
            refs[4 + dy][e] = refs[e][dy]


def pair_kernel(r0, r1, r2, r3, low, high):
    for dy, ref in enumerate((r0, r1, r2, r3)):
        (low, high)[dy // 2][dy % 2] = ref[...]


def assemble_kernel(own, swapped, z_same, z_cross, out):
    zhi = lax.axis_index("zhi")
    core = lax.axis_index("core")
    for piece, zz, cc in (
        (z_same, 1 - zhi, core),
        (z_cross, 1 - zhi, 1 - core),
        (own, zhi, core),
        (swapped, zhi, 1 - core),
    ):
        left = pl.multiple_of((zz * 2 + cc) * HEAD, HEAD)
        out[:, pl.ds(left, HEAD)] = piece[...]


def along(value, axis, by):
    return lax.ppermute(value, axis, [(i, (i + by) % 4) for i in range(4)])


def mirror(value, axes):
    size = 2 if isinstance(axes, str) else 4
    return lax.ppermute(value, axes, [(i, size - 1 - i) for i in range(size)])


Z_FLIPS = (None, "zlo", "zhi", ("zlo", "zhi"))


def layer(query, key, value, block_order):
    rows = query.shape[0]
    quarter = (4, rows, 2 * HEAD)
    q_quarter = (4, 2, rows, HEAD)
    *kv_z, keep, send = local_call(
        sort_kernel, [quarter] * 4 + [(4, 4, rows, HEAD)] * 2, (query, key, value)
    )
    kv_z = [kv_z[0]] + [mirror(kv_z[e], Z_FLIPS[e]) for e in (1, 3, 2)]
    kv_z = [kv_z[0], kv_z[1], kv_z[3], kv_z[2]]
    got = mirror(send, "core")
    q_z = local_call(join_kernel, [q_quarter] * 4, (keep, got))
    q_z = [q_z[0]] + [mirror(q_z[e], Z_FLIPS[e]) for e in (1, 2, 3)]

    kv_y = local_call(turn_kernel, [quarter] * 4, kv_z)
    kv_y = [kv_y[0]] + [along(kv_y[d], "y", d) for d in (1, 2, 3)]
    q_y = local_call(turn_kernel, [q_quarter] * 4, q_z)
    q_y = [q_y[0]] + [along(q_y[d], "y", d) for d in (1, 2, 3)]

    low, high = local_call(pair_kernel, [(2,) + quarter] * 2, kv_y)
    up_low = along(low, "x", 1)
    down_high = along(high, "x", -1)
    up_high = along(high, "x", 1)
    down_low = along(low, "x", -1)
    own_o = [mirror(low, "core"), mirror(high, "core")]
    far_low = along(up_low, "x", 1)
    far_high = along(down_high, "x", -1)
    up_o = [mirror(up_low, "core"), mirror(up_high, "core")]
    down_o = [mirror(down_low, "core"), mirror(down_high, "core")]
    far_o = [mirror(far_low, "core"), mirror(far_high, "core")]

    near = [((up_low, up_high), 1, 0), ((down_low, down_high), 3, 0)]
    near_o = [(up_o, 1, 1), (down_o, 3, 1)]
    far = [((far_low, far_high), 2, 0), (far_o, 2, 1)]

    def step(given, halves, carry, first=False, last=False):
        return attend(block_order, given, halves, carry, first, last)

    both = (REMOTE, LOCAL)
    state = step([((low, high), 0, 0), (own_o, 0, 1)], both, q_y, first=True)
    state = step(near, both, state)
    remote, local = state[:3], state[3:]
    remote = step(near_o, (REMOTE,), remote)
    same, cross = step(far, (REMOTE,), remote, last=True)
    z_same = mirror(same, "zhi")
    z_cross = mirror(cross, ("zhi", "core"))
    own, cross = step(near_o + far, (LOCAL,), local, last=True)
    swapped = mirror(cross, "core")
    (out,) = local_call(
        assemble_kernel, [(2 * BLK, 4 * HEAD)], (own, swapped, z_same, z_cross)
    )
    return out


def solution(mesh):
    fine = Mesh(mesh.devices.reshape(4, 2, 2, 4, 2), AXES)
    placed = P(("zhi", "x", "core", "y", "zlo"), None)
    return jax.shard_map(
        layer,
        mesh=fine,
        in_specs=(placed, placed, placed, P()),
        out_specs=P(("zhi", "x", "core"), ("y", "zlo")),
        check_vma=False,
    )
```

```python
import functools

import jax
import jax.numpy as jnp
from jax import lax
from jax.experimental import pallas as pl
from jax.experimental.pallas import tpu as pltpu
from jax.sharding import Mesh
from jax.sharding import PartitionSpec as P

HEAD = 128
BLK = 384
PIECE = 96
TILE = 256
HALF_BLOCKS = 4
TILES = HALF_BLOCKS * BLK // TILE
UNROLL = 4
SCORE_SCALE = 1.0 / (12.0 * 50.0)
CAP_LOG2E = 50.0 * 1.4426950408889634

AXES = ("y", "zlo", "zhi", "x", "core")
REMOTE, LOCAL = 0, 1


def attend_kernel(*refs, offsets, halves, first, last):
    n_shards = len(offsets)
    n_halves = len(halves)
    dummy_tile = n_halves * TILES
    refs = list(refs)
    order = refs.pop(0)
    kv = [refs.pop(0) for _ in range(n_shards)]
    if first:
        q_refs = [refs.pop(0) for _ in range(2)]
    else:
        states_in = [[refs.pop(0) for _ in range(3)] for _ in halves]
    if last:
        outs = [[refs.pop(0) for _ in range(2)] for _ in halves]
    else:
        states_out = [[refs.pop(0) for _ in range(3)] for _ in halves]
    qt, num, den, qpos, kbuf, vt = refs[:6]
    s_bufs = refs[6 : 6 + UNROLL]
    p_bufs = refs[6 + UNROLL : 6 + 2 * UNROLL]
    rows, q_seq, q_rank, kb_list, kb_start, kb_end, kb_seq = refs[6 + 2 * UNROLL :]

    x = lax.axis_index("x")
    core = lax.axis_index("core")
    zhi = lax.axis_index("zhi")

    lane = lax.broadcasted_iota(jnp.int32, (8, 128), 1)
    for n, half in enumerate(halves):
        zz = 1 - zhi if half == REMOTE else zhi
        seqs = []
        for slot in range(HALF_BLOCKS):
            yhi, flip = slot // 2, slot % 2
            cc = 1 - core if flip else core
            seqs.append(order[2 * (zz * 8 + x * 2 + cc) + yhi])
        for slot in range(HALF_BLOCKS):
            rank = jnp.int32(4 * n)
            for other in range(HALF_BLOCKS):
                if other != slot:
                    rank = rank + (seqs[other] < seqs[slot]).astype(jnp.int32)
            q_seq[rank] = seqs[slot]
            q_rank[4 * n + slot] = rank
    for g in range(2 * n_halves * TILES):
        base = q_seq[g // 3] * BLK + (g % 3) * 128
        qpos[g // 2, :, (g % 2) * 128 : (g % 2) * 128 + 128] = lane + base
    qpos[dummy_tile] = jnp.zeros((8, TILE), jnp.int32)

    if first:
        for n, half in enumerate(halves):
            zz = 1 - zhi if half == REMOTE else zhi
            for slot in range(HALF_BLOCKS):
                yhi, flip = slot // 2, slot % 2
                top = pl.multiple_of(q_rank[4 * n + slot] * BLK, BLK)
                for sub in range(4):
                    piece = q_refs[flip][yhi * 8 + sub * 2 + zz]
                    rows[pl.ds(top + sub * PIECE, PIECE), :] = piece
        for t in range(n_halves * TILES):
            qt[t] = rows[t * TILE : (t + 1) * TILE, :].T
            num[t] = jnp.zeros((HEAD, TILE), jnp.float32)
            den[t] = jnp.zeros((8, TILE), jnp.float32)
    else:
        for n in range(n_halves):
            for t in range(TILES):
                qt[n * TILES + t] = states_in[n][0][t]
                num[n * TILES + t] = states_in[n][1][t]
                den[n * TILES + t] = states_in[n][2][t]
    qt[dummy_tile] = jnp.zeros((HEAD, TILE), jnp.bfloat16)
    num[dummy_tile] = jnp.zeros((HEAD, TILE), jnp.float32)
    den[dummy_tile] = jnp.zeros((8, TILE), jnp.float32)

    count = jnp.int32(0)
    total = jnp.int32(0)
    for n, (dx, flip, yhi) in enumerate(offsets):
        xs = (x + (4 - dx)) % 4
        cs = 1 - core if flip else core
        for zz in range(2):
            kb = 2 * n + zz
            vals = []
            for sub in range(4):
                piece = kv[n][sub * 2 + zz]
                kbuf[kb, sub * PIECE : (sub + 1) * PIECE, :] = piece[:, :HEAD]
                vals.append(piece[:, HEAD:])
            vt[kb] = jnp.concatenate(vals, axis=0).T
            seq = order[2 * (zz * 8 + xs * 2 + cs) + yhi]
            for h in range(n_halves):
                below = jnp.int32(0)
                for rank in range(HALF_BLOCKS):
                    below = below + (q_seq[4 * h + rank] < seq).astype(jnp.int32)
                start = (3 * below) // 2
                kb_list[count] = jnp.int32(kb)
                kb_start[count] = start + h * TILES
                kb_end[count] = jnp.int32((h + 1) * TILES)
                kb_seq[count] = seq
                count = count + (start < TILES).astype(jnp.int32)
                total = total + (TILES - start)
    for extra in range(2 * UNROLL + 2):
        kb_list[count + extra] = jnp.int32(0)
        kb_start[count + extra] = jnp.int32(dummy_tile)
        kb_end[count + extra] = jnp.int32(0)
        kb_seq[count + extra] = jnp.int32(0)

    def after(item):
        j, t = item
        wrap = t + 1 >= kb_end[j]
        j = jnp.where(wrap, j + 1, j)
        return j, jnp.where(wrap, kb_start[j], t + 1)

    def score(item, s):
        j, t = item
        s[...] = jnp.dot(kbuf[kb_list[j]], qt[t], preferred_element_type=jnp.float32)

    row = lax.broadcasted_iota(jnp.int32, (8, TILE), 0)

    def weigh(item, s, p):
        j, t = item
        rel = qpos[t] - (kb_seq[j] * BLK + row)
        acc = None
        for r in range(0, BLK, 16):
            both = []
            for h in range(2):
                z = s[r + 8 * h : r + 8 * h + 8, :]
                w = jnp.exp2(CAP_LOG2E * jnp.tanh(z * SCORE_SCALE))
                w = jnp.where(rel >= r + 8 * h, w, 0.0)
                acc = w if acc is None else acc + w
                both.append(w)
            p[r : r + 16, :] = jnp.concatenate(both, axis=0).astype(jnp.bfloat16)
        den[t] = den[t] + acc

    def gather(item, p):
        j, t = item
        num[t] = num[t] + jnp.dot(vt[kb_list[j]], p[...], preferred_element_type=jnp.float32)

    items = [(jnp.int32(0), kb_start[0])]
    for _ in range(UNROLL - 1):
        items.append(after(items[-1]))
    for k in range(UNROLL):
        score(items[k], s_bufs[k])
    p_bufs[UNROLL - 1][...] = jnp.zeros((BLK, TILE), jnp.bfloat16)

    def body(_, state):
        cur, prev = state
        nxt = []
        item = cur[-1]
        for _ in range(UNROLL):
            item = after(item)
            nxt.append(item)
        for k in range(UNROLL):
            weigh(cur[k], s_bufs[k], p_bufs[k])
            score(nxt[k], s_bufs[k])
            if k == 0:
                gather(prev, p_bufs[UNROLL - 1])
            else:
                gather(cur[k - 1], p_bufs[k - 1])
        return tuple(nxt), cur[-1]

    idle = (count, jnp.int32(dummy_tile))
    _, tail = lax.fori_loop(0, (total + UNROLL - 1) // UNROLL, body, (tuple(items), idle))
    gather(tail, p_bufs[UNROLL - 1])

    if last:
        for t in range(n_halves * TILES):
            inv = 1.0 / jnp.sum(den[t], axis=0, keepdims=True)
            rows[t * TILE : (t + 1) * TILE, :] = (num[t] * inv).T.astype(jnp.bfloat16)
        for n in range(n_halves):
            for slot in range(HALF_BLOCKS):
                yhi, flip = slot // 2, slot % 2
                top = pl.multiple_of(q_rank[4 * n + slot] * BLK, BLK)
                outs[n][flip][yhi * BLK : (yhi + 1) * BLK, :] = rows[pl.ds(top, BLK), :]
    else:
        for n in range(n_halves):
            for t in range(TILES):
                states_out[n][0][t] = qt[n * TILES + t]
                states_out[n][1][t] = num[n * TILES + t]
                states_out[n][2][t] = den[n * TILES + t]


def attend(order, given, halves, carry, first, last):
    kvs = [piece for piece, _, _, _ in given]
    offsets = tuple(at for _, *at in given)
    vmem = pl.BlockSpec(memory_space=pltpu.VMEM)
    smem = pl.BlockSpec(memory_space=pltpu.SMEM)
    nb = 2 * len(given)
    tiles = TILES * len(halves)
    runs = nb * len(halves) + 2 * UNROLL + 4
    if last:
        out = (jax.ShapeDtypeStruct((2 * BLK, HEAD), jnp.bfloat16),) * (2 * len(halves))
    else:
        out = (
            jax.ShapeDtypeStruct((TILES, HEAD, TILE), jnp.bfloat16),
            jax.ShapeDtypeStruct((TILES, HEAD, TILE), jnp.float32),
            jax.ShapeDtypeStruct((TILES, 8, TILE), jnp.float32),
        ) * len(halves)
    inputs = [order, *kvs, *carry]
    return pl.pallas_call(
        functools.partial(attend_kernel, offsets=offsets, halves=halves, first=first, last=last),
        out_shape=out,
        in_specs=[smem] + [vmem] * (len(inputs) - 1),
        out_specs=(vmem,) * len(out),
        scratch_shapes=[
            pltpu.VMEM((tiles + 1, HEAD, TILE), jnp.bfloat16),
            pltpu.VMEM((tiles + 1, HEAD, TILE), jnp.float32),
            pltpu.VMEM((tiles + 1, 8, TILE), jnp.float32),
            pltpu.VMEM((tiles + 1, 8, TILE), jnp.int32),
            pltpu.VMEM((nb, BLK, HEAD), jnp.bfloat16),
            pltpu.VMEM((nb, HEAD, BLK), jnp.bfloat16),
            *[pltpu.VMEM((BLK, TILE), jnp.float32) for _ in range(UNROLL)],
            *[pltpu.VMEM((BLK, TILE), jnp.bfloat16) for _ in range(UNROLL)],
            pltpu.VMEM((tiles * TILE, HEAD), jnp.bfloat16),
            pltpu.SMEM((HALF_BLOCKS * len(halves),), jnp.int32),
            pltpu.SMEM((HALF_BLOCKS * len(halves),), jnp.int32),
            pltpu.SMEM((runs,), jnp.int32),
            pltpu.SMEM((runs,), jnp.int32),
            pltpu.SMEM((runs,), jnp.int32),
            pltpu.SMEM((runs,), jnp.int32),
        ],
        compiler_params=pltpu.CompilerParams(vmem_limit_bytes=36 * 1024 * 1024),
        cost_estimate=pl.CostEstimate(
            flops=len(given) * len(halves) * 600_000_000,
            transcendentals=0,
            bytes_accessed=4_000_000,
        ),
    )(*inputs)


def local_call(body, outs, inputs):
    vmem = pl.BlockSpec(memory_space=pltpu.VMEM)
    return pl.pallas_call(
        body,
        out_shape=tuple(jax.ShapeDtypeStruct(shape, jnp.bfloat16) for shape in outs),
        in_specs=[vmem] * len(inputs),
        out_specs=(vmem,) * len(outs),
        compiler_params=pltpu.CompilerParams(vmem_limit_bytes=8 * 1024 * 1024),
    )(*inputs)


def sort_kernel(query, key, value, out, sems):
    copies = []
    for head in range(16):
        for source, left, width in ((query, 0, 2 * HEAD), (key, 2 * HEAD, HEAD), (value, 3 * HEAD, HEAD)):
            copies.append(
                pltpu.make_async_copy(
                    source.at[:, head * width : (head + 1) * width],
                    out.at[head, :, left : left + width],
                    sems.at[len(copies)],
                )
            )
    for copy in copies:
        copy.start()
    for copy in copies:
        copy.wait()


def split_kernel(got, low, high, keep, send):
    core = lax.axis_index("core")
    mine = pl.multiple_of(core * HEAD, HEAD)
    other = pl.multiple_of((1 - core) * HEAD, HEAD)
    for n in range(16):
        (low, high)[n // 8][n % 8] = got[n, :, 2 * HEAD :]
        keep[n] = got[n, :, pl.ds(mine, HEAD)]
        send[n] = got[n, :, pl.ds(other, HEAD)]


def assemble_kernel(own, swapped, z_same, z_cross, out):
    zhi = lax.axis_index("zhi")
    core = lax.axis_index("core")
    for piece, zz, cc in (
        (z_same, 1 - zhi, core),
        (z_cross, 1 - zhi, 1 - core),
        (own, zhi, core),
        (swapped, zhi, 1 - core),
    ):
        left = pl.multiple_of((zz * 2 + cc) * HEAD, HEAD)
        out[:, pl.ds(left, HEAD)] = piece[...]


def along(value, axis, by):
    return lax.ppermute(value, axis, [(i, (i + by) % 4) for i in range(4)])


def mirror(value, axes):
    size = 2 if isinstance(axes, str) else 4
    return lax.ppermute(value, axes, [(i, size - 1 - i) for i in range(size)])


def layer(query, key, value, block_order):
    rows = query.shape[0]
    packed = pl.pallas_call(
        sort_kernel,
        out_shape=jax.ShapeDtypeStruct((16, rows, 4 * HEAD), jnp.bfloat16),
        in_specs=[pl.BlockSpec(memory_space=pltpu.HBM)] * 3,
        out_specs=pl.BlockSpec(memory_space=pltpu.VMEM),
        scratch_shapes=[pltpu.SemaphoreType.DMA((48,))],
        compiler_params=pltpu.CompilerParams(vmem_limit_bytes=8 * 1024 * 1024),
        name="k_sort",
    )(query, key, value)
    packed = lax.all_to_all(packed, ("y", "zlo", "zhi"), 0, 0)
    low, high, keep, send = local_call(
        split_kernel, [(8, rows, 2 * HEAD)] * 2 + [(16, rows, HEAD)] * 2, (packed,)
    )
    got = mirror(send, "core")
    up_low = along(low, "x", 1)
    down_high = along(high, "x", -1)
    up_high = along(high, "x", 1)
    down_low = along(low, "x", -1)
    far_low = along(up_low, "x", 1)
    far_high = along(down_high, "x", -1)

    def swap(half):
        return mirror(half, "core")

    own = [(low, 0, 0, 0), (high, 0, 0, 1)]
    own += [(swap(low), 0, 1, 0), (swap(high), 0, 1, 1)]
    near_a = [(up_low, 1, 0, 0), (down_high, 3, 0, 1)]
    near_b = [(up_high, 1, 0, 1), (down_low, 3, 0, 0)]
    near_b += [(swap(up_low), 1, 1, 0), (swap(down_high), 3, 1, 1)]
    near_c = [(swap(up_high), 1, 1, 1), (swap(down_low), 3, 1, 0)]
    far = [(far_low, 2, 0, 0), (far_high, 2, 0, 1)]
    far += [(swap(far_low), 2, 1, 0), (swap(far_high), 2, 1, 1)]

    def step(given, halves, carry, first=False, last=False):
        return attend(block_order, given, halves, carry, first, last)

    both = (REMOTE, LOCAL)
    state = step(own, both, (keep, got), first=True)
    state = step(near_a, both, state)
    remote, local = state[:3], state[3:]
    remote = step(near_b, (REMOTE,), remote)
    remote = step(near_c, (REMOTE,), remote)
    same, cross = step(far, (REMOTE,), remote, last=True)
    z_same = mirror(same, "zhi")
    z_cross = mirror(cross, ("zhi", "core"))
    mine, cross = step(near_b + near_c + far, (LOCAL,), local, last=True)
    swapped = mirror(cross, "core")
    (out,) = local_call(
        assemble_kernel, [(2 * BLK, 4 * HEAD)], (mine, swapped, z_same, z_cross)
    )
    return out


def solution(mesh):
    fine = Mesh(mesh.devices.reshape(4, 2, 2, 4, 2), AXES)
    placed = P(("zhi", "x", "core", "y", "zlo"), None)
    return jax.shard_map(
        layer,
        mesh=fine,
        in_specs=(placed, placed, placed, P()),
        out_specs=P(("zhi", "x", "core"), ("y", "zlo")),
        check_vma=False,
    )
```

```python
import functools

import jax
import jax.numpy as jnp
from jax import lax
from jax.experimental import pallas as pl
from jax.experimental.pallas import tpu as pltpu
from jax.sharding import Mesh
from jax.sharding import PartitionSpec as P

HEAD = 128
BLK = 384
PIECE = 96
TILE = 256
HALF_BLOCKS = 4
TILES = HALF_BLOCKS * BLK // TILE
UNROLL = 4
SCORE_SCALE = 1.0 / (12.0 * 50.0)
CAP_LOG2E = 50.0 * 1.4426950408889634

AXES = ("y", "zlo", "zhi", "x", "core")
REMOTE, LOCAL = 0, 1


def attend_kernel(*refs, offsets, halves, first, last):
    n_shards = len(offsets)
    n_halves = len(halves)
    dummy_tile = n_halves * TILES
    refs = list(refs)
    order = refs.pop(0)
    kv = [refs.pop(0) for _ in range(n_shards)]
    if first:
        q_refs = [refs.pop(0) for _ in range(2)]
    else:
        states_in = [[refs.pop(0) for _ in range(3)] for _ in halves]
    if last:
        outs = [[refs.pop(0) for _ in range(2)] for _ in halves]
    else:
        states_out = [[refs.pop(0) for _ in range(3)] for _ in halves]
    qt, num, den, qpos, kbuf, vt = refs[:6]
    s_bufs = refs[6 : 6 + UNROLL]
    p_bufs = refs[6 + UNROLL : 6 + 2 * UNROLL]
    rows, q_seq, q_rank, kb_list, kb_start, kb_end, kb_seq = refs[6 + 2 * UNROLL :]

    x = lax.axis_index("x")
    core = lax.axis_index("core")
    zhi = lax.axis_index("zhi")

    lane = lax.broadcasted_iota(jnp.int32, (8, 128), 1)
    for n, half in enumerate(halves):
        zz = 1 - zhi if half == REMOTE else zhi
        seqs = []
        for slot in range(HALF_BLOCKS):
            yhi, flip = slot // 2, slot % 2
            cc = 1 - core if flip else core
            seqs.append(order[2 * (zz * 8 + x * 2 + cc) + yhi])
        for slot in range(HALF_BLOCKS):
            rank = jnp.int32(4 * n)
            for other in range(HALF_BLOCKS):
                if other != slot:
                    rank = rank + (seqs[other] < seqs[slot]).astype(jnp.int32)
            q_seq[rank] = seqs[slot]
            q_rank[4 * n + slot] = rank
    for g in range(2 * n_halves * TILES):
        base = q_seq[g // 3] * BLK + (g % 3) * 128
        qpos[g // 2, :, (g % 2) * 128 : (g % 2) * 128 + 128] = lane + base
    qpos[dummy_tile] = jnp.zeros((8, TILE), jnp.int32)

    if first:
        for n, half in enumerate(halves):
            zz = 1 - zhi if half == REMOTE else zhi
            for slot in range(HALF_BLOCKS):
                yhi, flip = slot // 2, slot % 2
                top = pl.multiple_of(q_rank[4 * n + slot] * BLK, BLK)
                for sub in range(4):
                    piece = q_refs[flip][yhi * 8 + sub * 2 + zz]
                    rows[pl.ds(top + sub * PIECE, PIECE), :] = piece
        for t in range(n_halves * TILES):
            qt[t] = rows[t * TILE : (t + 1) * TILE, :].T
            num[t] = jnp.zeros((HEAD, TILE), jnp.float32)
            den[t] = jnp.zeros((8, TILE), jnp.float32)
    else:
        for n in range(n_halves):
            for t in range(TILES):
                qt[n * TILES + t] = states_in[n][0][t]
                num[n * TILES + t] = states_in[n][1][t]
                den[n * TILES + t] = states_in[n][2][t]
    qt[dummy_tile] = jnp.zeros((HEAD, TILE), jnp.bfloat16)
    num[dummy_tile] = jnp.zeros((HEAD, TILE), jnp.float32)
    den[dummy_tile] = jnp.zeros((8, TILE), jnp.float32)

    count = jnp.int32(0)
    total = jnp.int32(0)
    for n, (dx, flip, yhi) in enumerate(offsets):
        xs = (x + (4 - dx)) % 4
        cs = 1 - core if flip else core
        for zz in range(2):
            kb = 2 * n + zz
            vals = []
            for sub in range(4):
                piece = kv[n][sub * 2 + zz]
                kbuf[kb, sub * PIECE : (sub + 1) * PIECE, :] = piece[:, :HEAD]
                vals.append(piece[:, HEAD:])
            vt[kb] = jnp.concatenate(vals, axis=0).T
            seq = order[2 * (zz * 8 + xs * 2 + cs) + yhi]
            for h in range(n_halves):
                below = jnp.int32(0)
                for rank in range(HALF_BLOCKS):
                    below = below + (q_seq[4 * h + rank] < seq).astype(jnp.int32)
                start = (3 * below) // 2
                kb_list[count] = jnp.int32(kb)
                kb_start[count] = start + h * TILES
                kb_end[count] = jnp.int32((h + 1) * TILES)
                kb_seq[count] = seq
                count = count + (start < TILES).astype(jnp.int32)
                total = total + (TILES - start)
    for extra in range(2 * UNROLL + 2):
        kb_list[count + extra] = jnp.int32(0)
        kb_start[count + extra] = jnp.int32(dummy_tile)
        kb_end[count + extra] = jnp.int32(0)
        kb_seq[count + extra] = jnp.int32(0)

    def after(item):
        j, t = item
        wrap = t + 1 >= kb_end[j]
        j = jnp.where(wrap, j + 1, j)
        return j, jnp.where(wrap, kb_start[j], t + 1)

    def score(item, s):
        j, t = item
        s[...] = jnp.dot(kbuf[kb_list[j]], qt[t], preferred_element_type=jnp.float32)

    row = lax.broadcasted_iota(jnp.int32, (8, TILE), 0)

    def weigh(item, s, p):
        j, t = item
        rel = qpos[t] - (kb_seq[j] * BLK + row)
        acc = None
        for r in range(0, BLK, 16):
            both = []
            for h in range(2):
                z = s[r + 8 * h : r + 8 * h + 8, :]
                w = jnp.exp2(CAP_LOG2E * jnp.tanh(z * SCORE_SCALE))
                w = jnp.where(rel >= r + 8 * h, w, 0.0)
                acc = w if acc is None else acc + w
                both.append(w)
            p[r : r + 16, :] = jnp.concatenate(both, axis=0).astype(jnp.bfloat16)
        den[t] = den[t] + acc

    def gather(item, p):
        j, t = item
        num[t] = num[t] + jnp.dot(vt[kb_list[j]], p[...], preferred_element_type=jnp.float32)

    items = [(jnp.int32(0), kb_start[0])]
    for _ in range(UNROLL - 1):
        items.append(after(items[-1]))
    for k in range(UNROLL):
        score(items[k], s_bufs[k])
    p_bufs[UNROLL - 1][...] = jnp.zeros((BLK, TILE), jnp.bfloat16)

    def body(_, state):
        cur, prev = state
        nxt = []
        item = cur[-1]
        for _ in range(UNROLL):
            item = after(item)
            nxt.append(item)
        for k in range(UNROLL):
            weigh(cur[k], s_bufs[k], p_bufs[k])
            score(nxt[k], s_bufs[k])
            if k == 0:
                gather(prev, p_bufs[UNROLL - 1])
            else:
                gather(cur[k - 1], p_bufs[k - 1])
        return tuple(nxt), cur[-1]

    idle = (count, jnp.int32(dummy_tile))
    _, tail = lax.fori_loop(0, (total + UNROLL - 1) // UNROLL, body, (tuple(items), idle))
    gather(tail, p_bufs[UNROLL - 1])

    if last:
        for t in range(n_halves * TILES):
            inv = 1.0 / jnp.sum(den[t], axis=0, keepdims=True)
            rows[t * TILE : (t + 1) * TILE, :] = (num[t] * inv).T.astype(jnp.bfloat16)
        for n in range(n_halves):
            for slot in range(HALF_BLOCKS):
                yhi, flip = slot // 2, slot % 2
                top = pl.multiple_of(q_rank[4 * n + slot] * BLK, BLK)
                outs[n][flip][yhi * BLK : (yhi + 1) * BLK, :] = rows[pl.ds(top, BLK), :]
    else:
        for n in range(n_halves):
            for t in range(TILES):
                states_out[n][0][t] = qt[n * TILES + t]
                states_out[n][1][t] = num[n * TILES + t]
                states_out[n][2][t] = den[n * TILES + t]


def attend(order, given, halves, carry, first, last):
    kvs = [piece for piece, _, _, _ in given]
    offsets = tuple(at for _, *at in given)
    vmem = pl.BlockSpec(memory_space=pltpu.VMEM)
    smem = pl.BlockSpec(memory_space=pltpu.SMEM)
    nb = 2 * len(given)
    tiles = TILES * len(halves)
    runs = nb * len(halves) + 2 * UNROLL + 4
    if last:
        out = (jax.ShapeDtypeStruct((2 * BLK, HEAD), jnp.bfloat16),) * (2 * len(halves))
    else:
        out = (
            jax.ShapeDtypeStruct((TILES, HEAD, TILE), jnp.bfloat16),
            jax.ShapeDtypeStruct((TILES, HEAD, TILE), jnp.float32),
            jax.ShapeDtypeStruct((TILES, 8, TILE), jnp.float32),
        ) * len(halves)
    inputs = [order, *kvs, *carry]
    return pl.pallas_call(
        functools.partial(attend_kernel, offsets=offsets, halves=halves, first=first, last=last),
        out_shape=out,
        in_specs=[smem] + [vmem] * (len(inputs) - 1),
        out_specs=(vmem,) * len(out),
        scratch_shapes=[
            pltpu.VMEM((tiles + 1, HEAD, TILE), jnp.bfloat16),
            pltpu.VMEM((tiles + 1, HEAD, TILE), jnp.float32),
            pltpu.VMEM((tiles + 1, 8, TILE), jnp.float32),
            pltpu.VMEM((tiles + 1, 8, TILE), jnp.int32),
            pltpu.VMEM((nb, BLK, HEAD), jnp.bfloat16),
            pltpu.VMEM((nb, HEAD, BLK), jnp.bfloat16),
            *[pltpu.VMEM((BLK, TILE), jnp.float32) for _ in range(UNROLL)],
            *[pltpu.VMEM((BLK, TILE), jnp.bfloat16) for _ in range(UNROLL)],
            pltpu.VMEM((tiles * TILE, HEAD), jnp.bfloat16),
            pltpu.SMEM((HALF_BLOCKS * len(halves),), jnp.int32),
            pltpu.SMEM((HALF_BLOCKS * len(halves),), jnp.int32),
            pltpu.SMEM((runs,), jnp.int32),
            pltpu.SMEM((runs,), jnp.int32),
            pltpu.SMEM((runs,), jnp.int32),
            pltpu.SMEM((runs,), jnp.int32),
        ],
        compiler_params=pltpu.CompilerParams(vmem_limit_bytes=28 * 1024 * 1024),
        cost_estimate=pl.CostEstimate(
            flops=len(given) * len(halves) * 600_000_000,
            transcendentals=0,
            bytes_accessed=4_000_000,
        ),
    )(*inputs)


def local_call(body, outs, inputs):
    vmem = pl.BlockSpec(memory_space=pltpu.VMEM)
    return pl.pallas_call(
        body,
        out_shape=tuple(jax.ShapeDtypeStruct(shape, jnp.bfloat16) for shape in outs),
        in_specs=[vmem] * len(inputs),
        out_specs=(vmem,) * len(outs),
        compiler_params=pltpu.CompilerParams(vmem_limit_bytes=8 * 1024 * 1024),
    )(*inputs)


def sort_kernel(query, key, value, out, sems):
    copies = []
    for head in range(16):
        for source, left, width in ((query, 0, 2 * HEAD), (key, 2 * HEAD, HEAD), (value, 3 * HEAD, HEAD)):
            copies.append(
                pltpu.make_async_copy(
                    source.at[:, head * width : (head + 1) * width],
                    out.at[head, :, left : left + width],
                    sems.at[len(copies)],
                )
            )
    for copy in copies:
        copy.start()
    for copy in copies:
        copy.wait()


def split_kernel(got, low, high, keep, send):
    core = lax.axis_index("core")
    mine = pl.multiple_of(core * HEAD, HEAD)
    other = pl.multiple_of((1 - core) * HEAD, HEAD)
    for n in range(16):
        (low, high)[n // 8][n % 8] = got[n, :, 2 * HEAD :]
        keep[n] = got[n, :, pl.ds(mine, HEAD)]
        send[n] = got[n, :, pl.ds(other, HEAD)]


def assemble_kernel(own, swapped, z_same, z_cross, out):
    zhi = lax.axis_index("zhi")
    core = lax.axis_index("core")
    for piece, zz, cc in (
        (z_same, 1 - zhi, core),
        (z_cross, 1 - zhi, 1 - core),
        (own, zhi, core),
        (swapped, zhi, 1 - core),
    ):
        left = pl.multiple_of((zz * 2 + cc) * HEAD, HEAD)
        out[:, pl.ds(left, HEAD)] = piece[...]


def along(value, axis, by):
    return lax.ppermute(value, axis, [(i, (i + by) % 4) for i in range(4)])


def mirror(value, axes):
    size = 2 if isinstance(axes, str) else 4
    return lax.ppermute(value, axes, [(i, size - 1 - i) for i in range(size)])


def layer(query, key, value, block_order):
    rows = query.shape[0]
    packed = pl.pallas_call(
        sort_kernel,
        out_shape=jax.ShapeDtypeStruct((16, rows, 4 * HEAD), jnp.bfloat16),
        in_specs=[pl.BlockSpec(memory_space=pltpu.HBM)] * 3,
        out_specs=pl.BlockSpec(memory_space=pltpu.HBM),
        scratch_shapes=[pltpu.SemaphoreType.DMA((48,))],
        compiler_params=pltpu.CompilerParams(vmem_limit_bytes=62 * 1024 * 1024),
        name="k_sort",
    )(query, key, value)
    packed = lax.all_to_all(packed, ("y", "zlo", "zhi"), 0, 0)
    low, high, keep, send = local_call(
        split_kernel, [(8, rows, 2 * HEAD)] * 2 + [(16, rows, HEAD)] * 2, (packed,)
    )
    got = mirror(send, "core")
    up_low = along(low, "x", 1)
    down_high = along(high, "x", -1)
    up_high = along(high, "x", 1)
    down_low = along(low, "x", -1)
    far_low = along(up_low, "x", 1)
    far_high = along(down_high, "x", -1)

    def swap(half):
        return mirror(half, "core")

    own = [(low, 0, 0, 0), (high, 0, 0, 1)]
    own += [(swap(low), 0, 1, 0), (swap(high), 0, 1, 1)]
    near = [(up_low, 1, 0, 0), (down_high, 3, 0, 1), (up_high, 1, 0, 1), (down_low, 3, 0, 0)]
    near_o = [(swap(up_low), 1, 1, 0), (swap(down_high), 3, 1, 1)]
    near_o += [(swap(up_high), 1, 1, 1), (swap(down_low), 3, 1, 0)]
    far = [(far_low, 2, 0, 0), (far_high, 2, 0, 1)]
    far += [(swap(far_low), 2, 1, 0), (swap(far_high), 2, 1, 1)]

    def step(given, halves, carry, first=False, last=False):
        return attend(block_order, given, halves, carry, first, last)

    both = (REMOTE, LOCAL)
    state = step(own, both, (keep, got), first=True)
    state = step(near, both, state)
    remote, local = state[:3], state[3:]
    same, cross = step(near_o + far, (REMOTE,), remote, last=True)
    z_same = mirror(same, "zhi")
    z_cross = mirror(cross, ("zhi", "core"))
    mine, cross = step(near_o + far, (LOCAL,), local, last=True)
    swapped = mirror(cross, "core")
    (out,) = local_call(assemble_kernel, [(2 * BLK, 4 * HEAD)], (mine, swapped, z_same, z_cross))
    return out


def solution(mesh):
    fine = Mesh(mesh.devices.reshape(4, 2, 2, 4, 2), AXES)
    placed = P(("zhi", "x", "core", "y", "zlo"), None)
    return jax.shard_map(
        layer,
        mesh=fine,
        in_specs=(placed, placed, placed, P()),
        out_specs=P(("zhi", "x", "core"), ("y", "zlo")),
        check_vma=False,
    )
```

```python
import functools

import jax
import jax.numpy as jnp
from jax import lax
from jax.experimental import pallas as pl
from jax.experimental.pallas import tpu as pltpu
from jax.sharding import Mesh
from jax.sharding import PartitionSpec as P

HEAD = 128
BLK = 384
PIECE = 96
TILE = 256
HALF_BLOCKS = 4
TILES = HALF_BLOCKS * BLK // TILE
UNROLL = 4
SCORE_SCALE = 1.0 / (12.0 * 50.0)
CAP_LOG2E = 50.0 * 1.4426950408889634

AXES = ("y", "zlo", "zhi", "x", "core")
REMOTE, LOCAL = 0, 1


def attend_kernel(*refs, offsets, halves, first, last):
    n_shards = len(offsets)
    n_halves = len(halves)
    dummy_tile = n_halves * TILES
    refs = list(refs)
    order = refs.pop(0)
    kv = [refs.pop(0) for _ in range(n_shards)]
    if first:
        q_refs = [refs.pop(0) for _ in range(2)]
    else:
        states_in = [[refs.pop(0) for _ in range(3)] for _ in halves]
    if last:
        outs = [[refs.pop(0) for _ in range(2)] for _ in halves]
    else:
        states_out = [[refs.pop(0) for _ in range(3)] for _ in halves]
    qt, num, den, qpos, kbuf, vt = refs[:6]
    s_bufs = refs[6 : 6 + UNROLL]
    p_bufs = refs[6 + UNROLL : 6 + 2 * UNROLL]
    rows, q_seq, q_rank, kb_list, kb_start, kb_end, kb_seq = refs[6 + 2 * UNROLL :]

    x = lax.axis_index("x")
    core = lax.axis_index("core")
    zhi = lax.axis_index("zhi")

    lane = lax.broadcasted_iota(jnp.int32, (8, 128), 1)
    for n, half in enumerate(halves):
        zz = 1 - zhi if half == REMOTE else zhi
        seqs = []
        for slot in range(HALF_BLOCKS):
            yhi, flip = slot // 2, slot % 2
            cc = 1 - core if flip else core
            seqs.append(order[2 * (zz * 8 + x * 2 + cc) + yhi])
        for slot in range(HALF_BLOCKS):
            rank = jnp.int32(4 * n)
            for other in range(HALF_BLOCKS):
                if other != slot:
                    rank = rank + (seqs[other] < seqs[slot]).astype(jnp.int32)
            q_seq[rank] = seqs[slot]
            q_rank[4 * n + slot] = rank
    for g in range(2 * n_halves * TILES):
        base = q_seq[g // 3] * BLK + (g % 3) * 128
        qpos[g // 2, :, (g % 2) * 128 : (g % 2) * 128 + 128] = lane + base
    qpos[dummy_tile] = jnp.zeros((8, TILE), jnp.int32)

    if first:
        for n, half in enumerate(halves):
            zz = 1 - zhi if half == REMOTE else zhi
            for slot in range(HALF_BLOCKS):
                yhi, flip = slot // 2, slot % 2
                top = pl.multiple_of(q_rank[4 * n + slot] * BLK, BLK)
                for sub in range(4):
                    piece = q_refs[flip][yhi * 8 + sub * 2 + zz]
                    rows[pl.ds(top + sub * PIECE, PIECE), :] = piece
        for t in range(n_halves * TILES):
            qt[t] = rows[t * TILE : (t + 1) * TILE, :].T
            num[t] = jnp.zeros((HEAD, TILE), jnp.float32)
            den[t] = jnp.zeros((8, TILE), jnp.float32)
    else:
        for n in range(n_halves):
            for t in range(TILES):
                qt[n * TILES + t] = states_in[n][0][t]
                num[n * TILES + t] = states_in[n][1][t]
                den[n * TILES + t] = states_in[n][2][t]
    qt[dummy_tile] = jnp.zeros((HEAD, TILE), jnp.bfloat16)
    num[dummy_tile] = jnp.zeros((HEAD, TILE), jnp.float32)
    den[dummy_tile] = jnp.zeros((8, TILE), jnp.float32)

    count = jnp.int32(0)
    total = jnp.int32(0)
    for n, (dx, flip, yhi) in enumerate(offsets):
        xs = (x + (4 - dx)) % 4
        cs = 1 - core if flip else core
        for zz in range(2):
            kb = 2 * n + zz
            vals = []
            for sub in range(4):
                piece = kv[n][sub * 2 + zz]
                kbuf[kb, sub * PIECE : (sub + 1) * PIECE, :] = piece[:, :HEAD]
                vals.append(piece[:, HEAD:])
            vt[kb] = jnp.concatenate(vals, axis=0).T
            seq = order[2 * (zz * 8 + xs * 2 + cs) + yhi]
            for h in range(n_halves):
                below = jnp.int32(0)
                for rank in range(HALF_BLOCKS):
                    below = below + (q_seq[4 * h + rank] < seq).astype(jnp.int32)
                start = (3 * below) // 2
                kb_list[count] = jnp.int32(kb)
                kb_start[count] = start + h * TILES
                kb_end[count] = jnp.int32((h + 1) * TILES)
                kb_seq[count] = seq
                count = count + (start < TILES).astype(jnp.int32)
                total = total + (TILES - start)
    for extra in range(2 * UNROLL + 2):
        kb_list[count + extra] = jnp.int32(0)
        kb_start[count + extra] = jnp.int32(dummy_tile)
        kb_end[count + extra] = jnp.int32(0)
        kb_seq[count + extra] = jnp.int32(0)

    def after(item):
        j, t = item
        wrap = t + 1 >= kb_end[j]
        j = jnp.where(wrap, j + 1, j)
        return j, jnp.where(wrap, kb_start[j], t + 1)

    def score(item, s):
        j, t = item
        s[...] = jnp.dot(kbuf[kb_list[j]], qt[t], preferred_element_type=jnp.float32)

    row = lax.broadcasted_iota(jnp.int32, (8, TILE), 0)

    def weigh(item, s, p):
        j, t = item
        rel = qpos[t] - (kb_seq[j] * BLK + row)
        acc = None
        for r in range(0, BLK, 16):
            both = []
            for h in range(2):
                z = s[r + 8 * h : r + 8 * h + 8, :]
                w = jnp.exp2(CAP_LOG2E * jnp.tanh(z * SCORE_SCALE))
                w = jnp.where(rel >= r + 8 * h, w, 0.0)
                acc = w if acc is None else acc + w
                both.append(w)
            p[r : r + 16, :] = jnp.concatenate(both, axis=0).astype(jnp.bfloat16)
        den[t] = den[t] + acc

    def gather(item, p):
        j, t = item
        num[t] = num[t] + jnp.dot(vt[kb_list[j]], p[...], preferred_element_type=jnp.float32)

    items = [(jnp.int32(0), kb_start[0])]
    for _ in range(UNROLL - 1):
        items.append(after(items[-1]))
    for k in range(UNROLL):
        score(items[k], s_bufs[k])
    p_bufs[UNROLL - 1][...] = jnp.zeros((BLK, TILE), jnp.bfloat16)

    def body(_, state):
        cur, prev = state
        nxt = []
        item = cur[-1]
        for _ in range(UNROLL):
            item = after(item)
            nxt.append(item)
        weigh(cur[0], s_bufs[0], p_bufs[0])
        weigh(cur[1], s_bufs[1], p_bufs[1])
        gather(prev, p_bufs[3])
        score(nxt[0], s_bufs[0])
        score(nxt[1], s_bufs[1])
        gather(cur[0], p_bufs[0])
        weigh(cur[2], s_bufs[2], p_bufs[2])
        score(nxt[2], s_bufs[2])
        weigh(cur[3], s_bufs[3], p_bufs[3])
        gather(cur[1], p_bufs[1])
        gather(cur[2], p_bufs[2])
        score(nxt[3], s_bufs[3])
        return tuple(nxt), cur[-1]

    idle = (count, jnp.int32(dummy_tile))
    _, tail = lax.fori_loop(0, (total + UNROLL - 1) // UNROLL, body, (tuple(items), idle))
    gather(tail, p_bufs[UNROLL - 1])

    if last:
        for t in range(n_halves * TILES):
            inv = 1.0 / jnp.sum(den[t], axis=0, keepdims=True)
            rows[t * TILE : (t + 1) * TILE, :] = (num[t] * inv).T.astype(jnp.bfloat16)
        for n in range(n_halves):
            for slot in range(HALF_BLOCKS):
                yhi, flip = slot // 2, slot % 2
                top = pl.multiple_of(q_rank[4 * n + slot] * BLK, BLK)
                outs[n][flip][yhi * BLK : (yhi + 1) * BLK, :] = rows[pl.ds(top, BLK), :]
    else:
        for n in range(n_halves):
            for t in range(TILES):
                states_out[n][0][t] = qt[n * TILES + t]
                states_out[n][1][t] = num[n * TILES + t]
                states_out[n][2][t] = den[n * TILES + t]


def attend(order, given, halves, carry, first, last):
    kvs = [piece for piece, _, _, _ in given]
    offsets = tuple(at for _, *at in given)
    vmem = pl.BlockSpec(memory_space=pltpu.VMEM)
    smem = pl.BlockSpec(memory_space=pltpu.SMEM)
    nb = 2 * len(given)
    tiles = TILES * len(halves)
    runs = nb * len(halves) + 2 * UNROLL + 4
    if last:
        out = (jax.ShapeDtypeStruct((2 * BLK, HEAD), jnp.bfloat16),) * (2 * len(halves))
    else:
        out = (
            jax.ShapeDtypeStruct((TILES, HEAD, TILE), jnp.bfloat16),
            jax.ShapeDtypeStruct((TILES, HEAD, TILE), jnp.float32),
            jax.ShapeDtypeStruct((TILES, 8, TILE), jnp.float32),
        ) * len(halves)
    inputs = [order, *kvs, *carry]
    return pl.pallas_call(
        functools.partial(attend_kernel, offsets=offsets, halves=halves, first=first, last=last),
        out_shape=out,
        in_specs=[smem] + [vmem] * (len(inputs) - 1),
        out_specs=(vmem,) * len(out),
        scratch_shapes=[
            pltpu.VMEM((tiles + 1, HEAD, TILE), jnp.bfloat16),
            pltpu.VMEM((tiles + 1, HEAD, TILE), jnp.float32),
            pltpu.VMEM((tiles + 1, 8, TILE), jnp.float32),
            pltpu.VMEM((tiles + 1, 8, TILE), jnp.int32),
            pltpu.VMEM((nb, BLK, HEAD), jnp.bfloat16),
            pltpu.VMEM((nb, HEAD, BLK), jnp.bfloat16),
            *[pltpu.VMEM((BLK, TILE), jnp.float32) for _ in range(UNROLL)],
            *[pltpu.VMEM((BLK, TILE), jnp.bfloat16) for _ in range(UNROLL)],
            pltpu.VMEM((tiles * TILE, HEAD), jnp.bfloat16),
            pltpu.SMEM((HALF_BLOCKS * len(halves),), jnp.int32),
            pltpu.SMEM((HALF_BLOCKS * len(halves),), jnp.int32),
            pltpu.SMEM((runs,), jnp.int32),
            pltpu.SMEM((runs,), jnp.int32),
            pltpu.SMEM((runs,), jnp.int32),
            pltpu.SMEM((runs,), jnp.int32),
        ],
        compiler_params=pltpu.CompilerParams(vmem_limit_bytes=28 * 1024 * 1024),
        cost_estimate=pl.CostEstimate(
            flops=len(given) * len(halves) * 600_000_000,
            transcendentals=0,
            bytes_accessed=4_000_000,
        ),
    )(*inputs)


def local_call(body, outs, inputs):
    vmem = pl.BlockSpec(memory_space=pltpu.VMEM)
    return pl.pallas_call(
        body,
        out_shape=tuple(jax.ShapeDtypeStruct(shape, jnp.bfloat16) for shape in outs),
        in_specs=[vmem] * len(inputs),
        out_specs=(vmem,) * len(outs),
        compiler_params=pltpu.CompilerParams(vmem_limit_bytes=8 * 1024 * 1024),
    )(*inputs)


def sort_kernel(query, key, value, out, q_rows, k_rows, v_rows, packed, sems):
    copies = [
        pltpu.make_async_copy(source, rows, sems.at[n])
        for n, (source, rows) in enumerate(((query, q_rows), (key, k_rows), (value, v_rows)))
    ]
    for copy in copies:
        copy.start()
    for copy in copies:
        copy.wait()
    for head in range(16):
        packed[head, :, : 2 * HEAD] = q_rows[:, 2 * head * HEAD : 2 * (head + 1) * HEAD]
        packed[head, :, 2 * HEAD : 3 * HEAD] = k_rows[:, head * HEAD : (head + 1) * HEAD]
        packed[head, :, 3 * HEAD :] = v_rows[:, head * HEAD : (head + 1) * HEAD]
    done = pltpu.make_async_copy(packed, out, sems.at[3])
    done.start()
    done.wait()


def split_kernel(got, low, high, keep, send):
    core = lax.axis_index("core")
    mine = pl.multiple_of(core * HEAD, HEAD)
    other = pl.multiple_of((1 - core) * HEAD, HEAD)
    for n in range(16):
        (low, high)[n // 8][n % 8] = got[n, :, 2 * HEAD :]
        keep[n] = got[n, :, pl.ds(mine, HEAD)]
        send[n] = got[n, :, pl.ds(other, HEAD)]


def assemble_kernel(own, swapped, z_same, z_cross, out):
    zhi = lax.axis_index("zhi")
    core = lax.axis_index("core")
    for piece, zz, cc in (
        (z_same, 1 - zhi, core),
        (z_cross, 1 - zhi, 1 - core),
        (own, zhi, core),
        (swapped, zhi, 1 - core),
    ):
        left = pl.multiple_of((zz * 2 + cc) * HEAD, HEAD)
        out[:, pl.ds(left, HEAD)] = piece[...]


def along(value, axis, by):
    return lax.ppermute(value, axis, [(i, (i + by) % 4) for i in range(4)])


def mirror(value, axes):
    size = 2 if isinstance(axes, str) else 4
    return lax.ppermute(value, axes, [(i, size - 1 - i) for i in range(size)])


def layer(query, key, value, block_order):
    rows = query.shape[0]
    packed = pl.pallas_call(
        sort_kernel,
        out_shape=jax.ShapeDtypeStruct((16, rows, 4 * HEAD), jnp.bfloat16),
        in_specs=[pl.BlockSpec(memory_space=pltpu.HBM)] * 3,
        out_specs=pl.BlockSpec(memory_space=pltpu.HBM),
        scratch_shapes=[
            pltpu.VMEM(query.shape, jnp.bfloat16),
            pltpu.VMEM(key.shape, jnp.bfloat16),
            pltpu.VMEM(value.shape, jnp.bfloat16),
            pltpu.VMEM((16, rows, 4 * HEAD), jnp.bfloat16),
            pltpu.SemaphoreType.DMA((4,)),
        ],
        compiler_params=pltpu.CompilerParams(vmem_limit_bytes=62 * 1024 * 1024),
        name="k_sort",
    )(query, key, value)
    packed = lax.all_to_all(packed, ("y", "zlo", "zhi"), 0, 0)
    low, high, keep, send = local_call(
        split_kernel, [(8, rows, 2 * HEAD)] * 2 + [(16, rows, HEAD)] * 2, (packed,)
    )
    got = mirror(send, "core")
    up_low = along(low, "x", 1)
    down_high = along(high, "x", -1)
    up_high = along(high, "x", 1)
    down_low = along(low, "x", -1)
    far_low = along(up_low, "x", 1)
    far_high = along(down_high, "x", -1)

    def swap(half):
        return mirror(half, "core")

    own = [(low, 0, 0, 0), (high, 0, 0, 1)]
    own += [(swap(low), 0, 1, 0), (swap(high), 0, 1, 1)]
    near = [(up_low, 1, 0, 0), (down_high, 3, 0, 1), (up_high, 1, 0, 1), (down_low, 3, 0, 0)]
    near_o = [(swap(up_low), 1, 1, 0), (swap(down_high), 3, 1, 1)]
    near_o += [(swap(up_high), 1, 1, 1), (swap(down_low), 3, 1, 0)]
    far = [(far_low, 2, 0, 0), (far_high, 2, 0, 1)]
    far += [(swap(far_low), 2, 1, 0), (swap(far_high), 2, 1, 1)]

    def step(given, halves, carry, first=False, last=False):
        return attend(block_order, given, halves, carry, first, last)

    both = (REMOTE, LOCAL)
    state = step(own, both, (keep, got), first=True)
    state = step(near, both, state)
    remote, local = state[:3], state[3:]
    remote = step(near_o, (REMOTE,), remote)
    same, cross = step(far, (REMOTE,), remote, last=True)
    z_same = mirror(same, "zhi")
    z_cross = mirror(cross, ("zhi", "core"))
    mine, cross = step(near_o + far, (LOCAL,), local, last=True)
    swapped = mirror(cross, "core")
    (out,) = local_call(assemble_kernel, [(2 * BLK, 4 * HEAD)], (mine, swapped, z_same, z_cross))
    return out


def solution(mesh):
    fine = Mesh(mesh.devices.reshape(4, 2, 2, 4, 2), AXES)
    placed = P(("zhi", "x", "core", "y", "zlo"), None)
    return jax.shard_map(
        layer,
        mesh=fine,
        in_specs=(placed, placed, placed, P()),
        out_specs=P(("zhi", "x", "core"), ("y", "zlo")),
        check_vma=False,
    )
```

```python
import functools

import jax
import jax.numpy as jnp
from jax import lax
from jax.experimental import pallas as pl
from jax.experimental.pallas import tpu as pltpu
from jax.sharding import Mesh
from jax.sharding import PartitionSpec as P

HEAD = 128
BLK = 384
PIECE = 96
TILE = 256
HALF_BLOCKS = 4
TILES = HALF_BLOCKS * BLK // TILE
UNROLL = 4
SCORE_SCALE = 1.0 / (12.0 * 50.0)
CAP_LOG2E = 50.0 * 1.4426950408889634

AXES = ("y", "zlo", "zhi", "x", "core")
REMOTE, LOCAL = 0, 1


def attend_kernel(*refs, offsets, halves, first, last):
    n_shards = len(offsets)
    n_halves = len(halves)
    dummy_tile = n_halves * TILES
    refs = list(refs)
    order = refs.pop(0)
    kv = [refs.pop(0) for _ in range(n_shards)]
    if first:
        q_refs = [refs.pop(0) for _ in range(2)]
    else:
        states_in = [[refs.pop(0) for _ in range(3)] for _ in halves]
    if last:
        outs = [[refs.pop(0) for _ in range(2)] for _ in halves]
    else:
        states_out = [[refs.pop(0) for _ in range(3)] for _ in halves]
    qt, num, den, qpos, kbuf, vt = refs[:6]
    s_bufs = refs[6 : 6 + UNROLL]
    p_bufs = refs[6 + UNROLL : 6 + 2 * UNROLL]
    rows, q_seq, q_rank, kb_list, kb_start, kb_end, kb_seq = refs[6 + 2 * UNROLL :]

    x = lax.axis_index("x")
    core = lax.axis_index("core")
    zhi = lax.axis_index("zhi")

    lane = lax.broadcasted_iota(jnp.int32, (8, 128), 1)
    for n, half in enumerate(halves):
        zz = 1 - zhi if half == REMOTE else zhi
        seqs = []
        for slot in range(HALF_BLOCKS):
            yhi, flip = slot // 2, slot % 2
            cc = 1 - core if flip else core
            seqs.append(order[2 * (zz * 8 + x * 2 + cc) + yhi])
        for slot in range(HALF_BLOCKS):
            rank = jnp.int32(4 * n)
            for other in range(HALF_BLOCKS):
                if other != slot:
                    rank = rank + (seqs[other] < seqs[slot]).astype(jnp.int32)
            q_seq[rank] = seqs[slot]
            q_rank[4 * n + slot] = rank
    for g in range(2 * n_halves * TILES):
        base = q_seq[g // 3] * BLK + (g % 3) * 128
        qpos[g // 2, :, (g % 2) * 128 : (g % 2) * 128 + 128] = lane + base
    qpos[dummy_tile] = jnp.zeros((8, TILE), jnp.int32)

    if first:
        for n, half in enumerate(halves):
            zz = 1 - zhi if half == REMOTE else zhi
            for slot in range(HALF_BLOCKS):
                yhi, flip = slot // 2, slot % 2
                top = pl.multiple_of(q_rank[4 * n + slot] * BLK, BLK)
                for sub in range(4):
                    piece = q_refs[flip][yhi * 8 + sub * 2 + zz]
                    rows[pl.ds(top + sub * PIECE, PIECE), :] = piece
        for t in range(n_halves * TILES):
            qt[t] = rows[t * TILE : (t + 1) * TILE, :].T
            num[t] = jnp.zeros((HEAD, TILE), jnp.float32)
            den[t] = jnp.zeros((8, TILE), jnp.float32)
    else:
        for n in range(n_halves):
            for t in range(TILES):
                qt[n * TILES + t] = states_in[n][0][t]
                num[n * TILES + t] = states_in[n][1][t]
                den[n * TILES + t] = states_in[n][2][t]
    qt[dummy_tile] = jnp.zeros((HEAD, TILE), jnp.bfloat16)
    num[dummy_tile] = jnp.zeros((HEAD, TILE), jnp.float32)
    den[dummy_tile] = jnp.zeros((8, TILE), jnp.float32)

    count = jnp.int32(0)
    total = jnp.int32(0)
    for n, (dx, flip, yhi) in enumerate(offsets):
        xs = (x + (4 - dx)) % 4
        cs = 1 - core if flip else core
        for zz in range(2):
            kb = 2 * n + zz
            vals = []
            for sub in range(4):
                piece = kv[n][sub * 2 + zz]
                kbuf[kb, sub * PIECE : (sub + 1) * PIECE, :] = piece[:, :HEAD]
                vals.append(piece[:, HEAD:])
            vt[kb] = jnp.concatenate(vals, axis=0).T
            seq = order[2 * (zz * 8 + xs * 2 + cs) + yhi]
            for h in range(n_halves):
                below = jnp.int32(0)
                for rank in range(HALF_BLOCKS):
                    below = below + (q_seq[4 * h + rank] < seq).astype(jnp.int32)
                start = (3 * below) // 2
                kb_list[count] = jnp.int32(kb)
                kb_start[count] = start + h * TILES
                kb_end[count] = jnp.int32((h + 1) * TILES)
                kb_seq[count] = seq
                count = count + (start < TILES).astype(jnp.int32)
                total = total + (TILES - start)
    for extra in range(2 * UNROLL + 2):
        kb_list[count + extra] = jnp.int32(0)
        kb_start[count + extra] = jnp.int32(dummy_tile)
        kb_end[count + extra] = jnp.int32(0)
        kb_seq[count + extra] = jnp.int32(0)

    def after(item):
        j, t = item
        wrap = t + 1 >= kb_end[j]
        j = jnp.where(wrap, j + 1, j)
        return j, jnp.where(wrap, kb_start[j], t + 1)

    def score(item, s):
        j, t = item
        s[...] = jnp.dot(kbuf[kb_list[j]], qt[t], preferred_element_type=jnp.float32)

    row = lax.broadcasted_iota(jnp.int32, (8, TILE), 0)

    def weigh(item, s, p):
        j, t = item
        rel = qpos[t] - (kb_seq[j] * BLK + row)
        acc = None
        for r in range(0, BLK, 16):
            both = []
            for h in range(2):
                z = s[r + 8 * h : r + 8 * h + 8, :]
                w = jnp.exp2(CAP_LOG2E * jnp.tanh(z * SCORE_SCALE))
                w = jnp.where(rel >= r + 8 * h, w, 0.0)
                acc = w if acc is None else acc + w
                both.append(w)
            p[r : r + 16, :] = jnp.concatenate(both, axis=0).astype(jnp.bfloat16)
        den[t] = den[t] + acc

    def gather(item, p):
        j, t = item
        num[t] = num[t] + jnp.dot(vt[kb_list[j]], p[...], preferred_element_type=jnp.float32)

    items = [(jnp.int32(0), kb_start[0])]
    for _ in range(UNROLL - 1):
        items.append(after(items[-1]))
    for k in range(UNROLL):
        score(items[k], s_bufs[k])
    p_bufs[UNROLL - 1][...] = jnp.zeros((BLK, TILE), jnp.bfloat16)

    def body(_, state):
        cur, prev = state
        nxt = []
        item = cur[-1]
        for _ in range(UNROLL):
            item = after(item)
            nxt.append(item)
        weigh(cur[0], s_bufs[0], p_bufs[0])
        weigh(cur[1], s_bufs[1], p_bufs[1])
        gather(prev, p_bufs[3])
        score(nxt[0], s_bufs[0])
        score(nxt[1], s_bufs[1])
        gather(cur[0], p_bufs[0])
        weigh(cur[2], s_bufs[2], p_bufs[2])
        score(nxt[2], s_bufs[2])
        weigh(cur[3], s_bufs[3], p_bufs[3])
        gather(cur[1], p_bufs[1])
        gather(cur[2], p_bufs[2])
        score(nxt[3], s_bufs[3])
        return tuple(nxt), cur[-1]

    idle = (count, jnp.int32(dummy_tile))
    _, tail = lax.fori_loop(0, (total + UNROLL - 1) // UNROLL, body, (tuple(items), idle))
    gather(tail, p_bufs[UNROLL - 1])

    if last:
        for t in range(n_halves * TILES):
            inv = 1.0 / jnp.sum(den[t], axis=0, keepdims=True)
            rows[t * TILE : (t + 1) * TILE, :] = (num[t] * inv).T.astype(jnp.bfloat16)
        for n in range(n_halves):
            for slot in range(HALF_BLOCKS):
                yhi, flip = slot // 2, slot % 2
                top = pl.multiple_of(q_rank[4 * n + slot] * BLK, BLK)
                outs[n][flip][yhi * BLK : (yhi + 1) * BLK, :] = rows[pl.ds(top, BLK), :]
    else:
        for n in range(n_halves):
            for t in range(TILES):
                states_out[n][0][t] = qt[n * TILES + t]
                states_out[n][1][t] = num[n * TILES + t]
                states_out[n][2][t] = den[n * TILES + t]


def attend(order, given, halves, carry, first, last):
    kvs = [piece for piece, _, _, _ in given]
    offsets = tuple(at for _, *at in given)
    vmem = pl.BlockSpec(memory_space=pltpu.VMEM)
    smem = pl.BlockSpec(memory_space=pltpu.SMEM)
    nb = 2 * len(given)
    tiles = TILES * len(halves)
    runs = nb * len(halves) + 2 * UNROLL + 4
    if last:
        out = (jax.ShapeDtypeStruct((2 * BLK, HEAD), jnp.bfloat16),) * (2 * len(halves))
    else:
        out = (
            jax.ShapeDtypeStruct((TILES, HEAD, TILE), jnp.bfloat16),
            jax.ShapeDtypeStruct((TILES, HEAD, TILE), jnp.float32),
            jax.ShapeDtypeStruct((TILES, 8, TILE), jnp.float32),
        ) * len(halves)
    inputs = [order, *kvs, *carry]
    return pl.pallas_call(
        functools.partial(attend_kernel, offsets=offsets, halves=halves, first=first, last=last),
        out_shape=out,
        in_specs=[smem] + [vmem] * (len(inputs) - 1),
        out_specs=(vmem,) * len(out),
        scratch_shapes=[
            pltpu.VMEM((tiles + 1, HEAD, TILE), jnp.bfloat16),
            pltpu.VMEM((tiles + 1, HEAD, TILE), jnp.float32),
            pltpu.VMEM((tiles + 1, 8, TILE), jnp.float32),
            pltpu.VMEM((tiles + 1, 8, TILE), jnp.int32),
            pltpu.VMEM((nb, BLK, HEAD), jnp.bfloat16),
            pltpu.VMEM((nb, HEAD, BLK), jnp.bfloat16),
            *[pltpu.VMEM((BLK, TILE), jnp.float32) for _ in range(UNROLL)],
            *[pltpu.VMEM((BLK, TILE), jnp.bfloat16) for _ in range(UNROLL)],
            pltpu.VMEM((tiles * TILE, HEAD), jnp.bfloat16),
            pltpu.SMEM((HALF_BLOCKS * len(halves),), jnp.int32),
            pltpu.SMEM((HALF_BLOCKS * len(halves),), jnp.int32),
            pltpu.SMEM((runs,), jnp.int32),
            pltpu.SMEM((runs,), jnp.int32),
            pltpu.SMEM((runs,), jnp.int32),
            pltpu.SMEM((runs,), jnp.int32),
        ],
        compiler_params=pltpu.CompilerParams(vmem_limit_bytes=28 * 1024 * 1024),
        cost_estimate=pl.CostEstimate(
            flops=len(given) * len(halves) * 600_000_000,
            transcendentals=0,
            bytes_accessed=4_000_000,
        ),
    )(*inputs)


def local_call(body, outs, inputs):
    vmem = pl.BlockSpec(memory_space=pltpu.VMEM)
    return pl.pallas_call(
        body,
        out_shape=tuple(jax.ShapeDtypeStruct(shape, jnp.bfloat16) for shape in outs),
        in_specs=[vmem] * len(inputs),
        out_specs=(vmem,) * len(outs),
        compiler_params=pltpu.CompilerParams(vmem_limit_bytes=8 * 1024 * 1024),
    )(*inputs)


def sort_kernel(query, key, value, out, q_rows, k_rows, v_rows, packed, sems):
    copies = [
        pltpu.make_async_copy(source, rows, sems.at[n])
        for n, (source, rows) in enumerate(((query, q_rows), (key, k_rows), (value, v_rows)))
    ]
    for copy in copies:
        copy.start()
    for copy in copies:
        copy.wait()
    for head in range(16):
        packed[head, :, : 2 * HEAD] = q_rows[:, 2 * head * HEAD : 2 * (head + 1) * HEAD]
        packed[head, :, 2 * HEAD : 3 * HEAD] = k_rows[:, head * HEAD : (head + 1) * HEAD]
        packed[head, :, 3 * HEAD :] = v_rows[:, head * HEAD : (head + 1) * HEAD]
    done = pltpu.make_async_copy(packed, out, sems.at[3])
    done.start()
    done.wait()


def split_kernel(got, low, high, keep, send):
    core = lax.axis_index("core")
    mine = pl.multiple_of(core * HEAD, HEAD)
    other = pl.multiple_of((1 - core) * HEAD, HEAD)
    for n in range(16):
        (low, high)[n // 8][n % 8] = got[n, :, 2 * HEAD :]
        keep[n] = got[n, :, pl.ds(mine, HEAD)]
        send[n] = got[n, :, pl.ds(other, HEAD)]


def assemble_kernel(own, swapped, z_same, z_cross, out):
    zhi = lax.axis_index("zhi")
    core = lax.axis_index("core")
    for piece, zz, cc in (
        (z_same, 1 - zhi, core),
        (z_cross, 1 - zhi, 1 - core),
        (own, zhi, core),
        (swapped, zhi, 1 - core),
    ):
        left = pl.multiple_of((zz * 2 + cc) * HEAD, HEAD)
        out[:, pl.ds(left, HEAD)] = piece[...]


def along(value, axis, by):
    return lax.ppermute(value, axis, [(i, (i + by) % 4) for i in range(4)])


def mirror(value, axes):
    size = 2 if isinstance(axes, str) else 4
    return lax.ppermute(value, axes, [(i, size - 1 - i) for i in range(size)])


def layer(query, key, value, block_order):
    rows = query.shape[0]
    packed = pl.pallas_call(
        sort_kernel,
        out_shape=jax.ShapeDtypeStruct((16, rows, 4 * HEAD), jnp.bfloat16),
        in_specs=[pl.BlockSpec(memory_space=pltpu.HBM)] * 3,
        out_specs=pl.BlockSpec(memory_space=pltpu.HBM),
        scratch_shapes=[
            pltpu.VMEM(query.shape, jnp.bfloat16),
            pltpu.VMEM(key.shape, jnp.bfloat16),
            pltpu.VMEM(value.shape, jnp.bfloat16),
            pltpu.VMEM((16, rows, 4 * HEAD), jnp.bfloat16),
            pltpu.SemaphoreType.DMA((4,)),
        ],
        compiler_params=pltpu.CompilerParams(vmem_limit_bytes=62 * 1024 * 1024),
        name="k_sort",
    )(query, key, value)
    packed = lax.all_to_all(packed, ("y", "zlo", "zhi"), 0, 0)
    low, high, keep, send = local_call(
        split_kernel, [(8, rows, 2 * HEAD)] * 2 + [(16, rows, HEAD)] * 2, (packed,)
    )
    got = mirror(send, "core")
    up_low = along(low, "x", 1)
    down_high = along(high, "x", -1)
    up_high = along(high, "x", 1)
    down_low = along(low, "x", -1)
    far_low = along(up_low, "x", 1)
    far_high = along(down_high, "x", -1)

    def swap(half):
        return mirror(half, "core")

    own = [(low, 0, 0, 0), (high, 0, 0, 1)]
    own += [(swap(low), 0, 1, 0), (swap(high), 0, 1, 1)]
    near = [(up_low, 1, 0, 0), (down_high, 3, 0, 1)]
    near += [(swap(up_low), 1, 1, 0), (swap(down_high), 3, 1, 1)]
    rest = [(up_high, 1, 0, 1), (down_low, 3, 0, 0)]
    rest += [(swap(up_high), 1, 1, 1), (swap(down_low), 3, 1, 0)]
    far = [(far_low, 2, 0, 0), (far_high, 2, 0, 1)]
    far += [(swap(far_low), 2, 1, 0), (swap(far_high), 2, 1, 1)]

    def step(given, halves, carry, first=False, last=False):
        return attend(block_order, given, halves, carry, first, last)

    both = (REMOTE, LOCAL)
    state = step(own, both, (keep, got), first=True)
    state = step(near, both, state)
    remote, local = state[:3], state[3:]
    remote = step(rest, (REMOTE,), remote)
    same, cross = step(far, (REMOTE,), remote, last=True)
    z_same = mirror(same, "zhi")
    z_cross = mirror(cross, ("zhi", "core"))
    mine, cross = step(rest + far, (LOCAL,), local, last=True)
    swapped = mirror(cross, "core")
    (out,) = local_call(
        assemble_kernel, [(2 * BLK, 4 * HEAD)], (mine, swapped, z_same, z_cross)
    )
    return out


def solution(mesh):
    fine = Mesh(mesh.devices.reshape(4, 2, 2, 4, 2), AXES)
    placed = P(("zhi", "x", "core", "y", "zlo"), None)
    return jax.shard_map(
        layer,
        mesh=fine,
        in_specs=(placed, placed, placed, P()),
        out_specs=P(("zhi", "x", "core"), ("y", "zlo")),
        check_vma=False,
    )
```

```python
import functools

import jax
import jax.numpy as jnp
from jax import lax
from jax.experimental import pallas as pl
from jax.experimental.pallas import tpu as pltpu
from jax.sharding import Mesh
from jax.sharding import PartitionSpec as P

HEAD = 128
BLK = 384
PIECE = 96
TILE = 256
HALF_BLOCKS = 4
TILES = HALF_BLOCKS * BLK // TILE
UNROLL = 4
SCORE_SCALE = 1.0 / (12.0 * 50.0)
CAP_LOG2E = 50.0 * 1.4426950408889634

AXES = ("y", "zlo", "zhi", "x", "core")
REMOTE, LOCAL = 0, 1


def attend_kernel(*refs, offsets, halves, first, last):
    n_shards = len(offsets)
    n_halves = len(halves)
    dummy_tile = n_halves * TILES
    refs = list(refs)
    order = refs.pop(0)
    kv = [refs.pop(0) for _ in range(n_shards)]
    if first:
        q_refs = [refs.pop(0) for _ in range(2)]
    else:
        states_in = [[refs.pop(0) for _ in range(3)] for _ in halves]
    if last:
        outs = [[refs.pop(0) for _ in range(2)] for _ in halves]
    else:
        states_out = [[refs.pop(0) for _ in range(3)] for _ in halves]
    qt, num, den, qpos, kbuf, vt = refs[:6]
    s_bufs = refs[6 : 6 + UNROLL]
    p_bufs = refs[6 + UNROLL : 6 + 2 * UNROLL]
    rows, q_seq, q_rank, kb_list, kb_start, kb_end, kb_seq = refs[6 + 2 * UNROLL :]

    x = lax.axis_index("x")
    core = lax.axis_index("core")
    zhi = lax.axis_index("zhi")

    lane = lax.broadcasted_iota(jnp.int32, (8, 128), 1)
    for n, half in enumerate(halves):
        zz = 1 - zhi if half == REMOTE else zhi
        seqs = []
        for slot in range(HALF_BLOCKS):
            yhi, flip = slot // 2, slot % 2
            cc = 1 - core if flip else core
            seqs.append(order[2 * (zz * 8 + x * 2 + cc) + yhi])
        for slot in range(HALF_BLOCKS):
            rank = jnp.int32(4 * n)
            for other in range(HALF_BLOCKS):
                if other != slot:
                    rank = rank + (seqs[other] < seqs[slot]).astype(jnp.int32)
            q_seq[rank] = seqs[slot]
            q_rank[4 * n + slot] = rank
    for g in range(2 * n_halves * TILES):
        base = q_seq[g // 3] * BLK + (g % 3) * 128
        qpos[g // 2, :, (g % 2) * 128 : (g % 2) * 128 + 128] = lane + base
    qpos[dummy_tile] = jnp.zeros((8, TILE), jnp.int32)

    if first:
        for n, half in enumerate(halves):
            zz = 1 - zhi if half == REMOTE else zhi
            for slot in range(HALF_BLOCKS):
                yhi, flip = slot // 2, slot % 2
                top = pl.multiple_of(q_rank[4 * n + slot] * BLK, BLK)
                for sub in range(4):
                    piece = q_refs[flip][yhi * 8 + sub * 2 + zz]
                    rows[pl.ds(top + sub * PIECE, PIECE), :] = piece
        for t in range(n_halves * TILES):
            qt[t] = rows[t * TILE : (t + 1) * TILE, :].T
            num[t] = jnp.zeros((HEAD, TILE), jnp.float32)
            den[t] = jnp.zeros((8, TILE), jnp.float32)
    else:
        for n in range(n_halves):
            for t in range(TILES):
                qt[n * TILES + t] = states_in[n][0][t]
                num[n * TILES + t] = states_in[n][1][t]
                den[n * TILES + t] = states_in[n][2][t]
    qt[dummy_tile] = jnp.zeros((HEAD, TILE), jnp.bfloat16)
    num[dummy_tile] = jnp.zeros((HEAD, TILE), jnp.float32)
    den[dummy_tile] = jnp.zeros((8, TILE), jnp.float32)

    count = jnp.int32(0)
    total = jnp.int32(0)
    for n, (dx, flip, yhi) in enumerate(offsets):
        xs = (x + (4 - dx)) % 4
        cs = 1 - core if flip else core
        for zz in range(2):
            kb = 2 * n + zz
            vals = []
            for sub in range(4):
                piece = kv[n][sub * 2 + zz]
                kbuf[kb, sub * PIECE : (sub + 1) * PIECE, :] = piece[:, :HEAD]
                vals.append(piece[:, HEAD:])
            vt[kb] = jnp.concatenate(vals, axis=0).T
            seq = order[2 * (zz * 8 + xs * 2 + cs) + yhi]
            for h in range(n_halves):
                below = jnp.int32(0)
                for rank in range(HALF_BLOCKS):
                    below = below + (q_seq[4 * h + rank] < seq).astype(jnp.int32)
                start = (3 * below) // 2
                kb_list[count] = jnp.int32(kb)
                kb_start[count] = start + h * TILES
                kb_end[count] = jnp.int32((h + 1) * TILES)
                kb_seq[count] = seq
                count = count + (start < TILES).astype(jnp.int32)
                total = total + (TILES - start)
    for extra in range(2 * UNROLL + 2):
        kb_list[count + extra] = jnp.int32(0)
        kb_start[count + extra] = jnp.int32(dummy_tile)
        kb_end[count + extra] = jnp.int32(0)
        kb_seq[count + extra] = jnp.int32(0)

    def after(item):
        j, t = item
        wrap = t + 1 >= kb_end[j]
        j = jnp.where(wrap, j + 1, j)
        return j, jnp.where(wrap, kb_start[j], t + 1)

    def score(item, s):
        j, t = item
        s[...] = jnp.dot(kbuf[kb_list[j]], qt[t], preferred_element_type=jnp.float32)

    row = lax.broadcasted_iota(jnp.int32, (8, TILE), 0)

    def weigh(item, s, p):
        j, t = item
        rel = qpos[t] - (kb_seq[j] * BLK + row)
        acc = None
        for r in range(0, BLK, 16):
            both = []
            for h in range(2):
                z = s[r + 8 * h : r + 8 * h + 8, :]
                w = jnp.exp2(CAP_LOG2E * jnp.tanh(z * SCORE_SCALE))
                w = jnp.where(rel >= r + 8 * h, w, 0.0)
                acc = w if acc is None else acc + w
                both.append(w)
            p[r : r + 16, :] = jnp.concatenate(both, axis=0).astype(jnp.bfloat16)
        den[t] = den[t] + acc

    def gather(item, p):
        j, t = item
        num[t] = num[t] + jnp.dot(vt[kb_list[j]], p[...], preferred_element_type=jnp.float32)

    items = [(jnp.int32(0), kb_start[0])]
    for _ in range(UNROLL - 1):
        items.append(after(items[-1]))
    for k in range(UNROLL):
        score(items[k], s_bufs[k])
    p_bufs[UNROLL - 1][...] = jnp.zeros((BLK, TILE), jnp.bfloat16)

    def body(_, state):
        cur, prev = state
        nxt = []
        item = cur[-1]
        for _ in range(UNROLL):
            item = after(item)
            nxt.append(item)
        weigh(cur[0], s_bufs[0], p_bufs[0])
        weigh(cur[1], s_bufs[1], p_bufs[1])
        gather(prev, p_bufs[3])
        score(nxt[0], s_bufs[0])
        score(nxt[1], s_bufs[1])
        gather(cur[0], p_bufs[0])
        weigh(cur[2], s_bufs[2], p_bufs[2])
        score(nxt[2], s_bufs[2])
        weigh(cur[3], s_bufs[3], p_bufs[3])
        gather(cur[1], p_bufs[1])
        gather(cur[2], p_bufs[2])
        score(nxt[3], s_bufs[3])
        return tuple(nxt), cur[-1]

    idle = (count, jnp.int32(dummy_tile))
    _, tail = lax.fori_loop(0, (total + UNROLL - 1) // UNROLL, body, (tuple(items), idle))
    gather(tail, p_bufs[UNROLL - 1])

    if last:
        for t in range(n_halves * TILES):
            inv = 1.0 / jnp.sum(den[t], axis=0, keepdims=True)
            rows[t * TILE : (t + 1) * TILE, :] = (num[t] * inv).T.astype(jnp.bfloat16)
        for n in range(n_halves):
            for slot in range(HALF_BLOCKS):
                yhi, flip = slot // 2, slot % 2
                top = pl.multiple_of(q_rank[4 * n + slot] * BLK, BLK)
                outs[n][flip][yhi * BLK : (yhi + 1) * BLK, :] = rows[pl.ds(top, BLK), :]
    else:
        for n in range(n_halves):
            for t in range(TILES):
                states_out[n][0][t] = qt[n * TILES + t]
                states_out[n][1][t] = num[n * TILES + t]
                states_out[n][2][t] = den[n * TILES + t]


def attend(order, given, halves, carry, first, last):
    kvs = [piece for piece, _, _, _ in given]
    offsets = tuple(at for _, *at in given)
    vmem = pl.BlockSpec(memory_space=pltpu.VMEM)
    smem = pl.BlockSpec(memory_space=pltpu.SMEM)
    nb = 2 * len(given)
    tiles = TILES * len(halves)
    runs = nb * len(halves) + 2 * UNROLL + 4
    if last:
        out = (jax.ShapeDtypeStruct((2 * BLK, HEAD), jnp.bfloat16),) * (2 * len(halves))
    else:
        out = (
            jax.ShapeDtypeStruct((TILES, HEAD, TILE), jnp.bfloat16),
            jax.ShapeDtypeStruct((TILES, HEAD, TILE), jnp.float32),
            jax.ShapeDtypeStruct((TILES, 8, TILE), jnp.float32),
        ) * len(halves)
    inputs = [order, *kvs, *carry]
    return pl.pallas_call(
        functools.partial(attend_kernel, offsets=offsets, halves=halves, first=first, last=last),
        out_shape=out,
        in_specs=[smem] + [vmem] * (len(inputs) - 1),
        out_specs=(vmem,) * len(out),
        scratch_shapes=[
            pltpu.VMEM((tiles + 1, HEAD, TILE), jnp.bfloat16),
            pltpu.VMEM((tiles + 1, HEAD, TILE), jnp.float32),
            pltpu.VMEM((tiles + 1, 8, TILE), jnp.float32),
            pltpu.VMEM((tiles + 1, 8, TILE), jnp.int32),
            pltpu.VMEM((nb, BLK, HEAD), jnp.bfloat16),
            pltpu.VMEM((nb, HEAD, BLK), jnp.bfloat16),
            *[pltpu.VMEM((BLK, TILE), jnp.float32) for _ in range(UNROLL)],
            *[pltpu.VMEM((BLK, TILE), jnp.bfloat16) for _ in range(UNROLL)],
            pltpu.VMEM((tiles * TILE, HEAD), jnp.bfloat16),
            pltpu.SMEM((HALF_BLOCKS * len(halves),), jnp.int32),
            pltpu.SMEM((HALF_BLOCKS * len(halves),), jnp.int32),
            pltpu.SMEM((runs,), jnp.int32),
            pltpu.SMEM((runs,), jnp.int32),
            pltpu.SMEM((runs,), jnp.int32),
            pltpu.SMEM((runs,), jnp.int32),
        ],
        compiler_params=pltpu.CompilerParams(vmem_limit_bytes=28 * 1024 * 1024),
        cost_estimate=pl.CostEstimate(
            flops=len(given) * len(halves) * 600_000_000,
            transcendentals=0,
            bytes_accessed=4_000_000,
        ),
    )(*inputs)


def local_call(body, outs, inputs):
    vmem = pl.BlockSpec(memory_space=pltpu.VMEM)
    return pl.pallas_call(
        body,
        out_shape=tuple(jax.ShapeDtypeStruct(shape, jnp.bfloat16) for shape in outs),
        in_specs=[vmem] * len(inputs),
        out_specs=(vmem,) * len(outs),
        compiler_params=pltpu.CompilerParams(vmem_limit_bytes=8 * 1024 * 1024),
    )(*inputs)


def sort_kernel(query, key, value, out, q_rows, k_rows, v_rows, packed, sems):
    copies = [
        pltpu.make_async_copy(source, rows, sems.at[n])
        for n, (source, rows) in enumerate(((query, q_rows), (key, k_rows), (value, v_rows)))
    ]
    for copy in copies:
        copy.start()
    for copy in copies:
        copy.wait()
    for head in range(16):
        packed[head, :, : 2 * HEAD] = q_rows[:, 2 * head * HEAD : 2 * (head + 1) * HEAD]
        packed[head, :, 2 * HEAD : 3 * HEAD] = k_rows[:, head * HEAD : (head + 1) * HEAD]
        packed[head, :, 3 * HEAD :] = v_rows[:, head * HEAD : (head + 1) * HEAD]
    done = pltpu.make_async_copy(packed, out, sems.at[3])
    done.start()
    done.wait()


def split_kernel(got, low, high, keep, send):
    core = lax.axis_index("core")
    mine = pl.multiple_of(core * HEAD, HEAD)
    other = pl.multiple_of((1 - core) * HEAD, HEAD)
    for n in range(16):
        (low, high)[n // 8][n % 8] = got[n, :, 2 * HEAD :]
        keep[n] = got[n, :, pl.ds(mine, HEAD)]
        send[n] = got[n, :, pl.ds(other, HEAD)]


def assemble_kernel(own, swapped, z_same, z_cross, out):
    zhi = lax.axis_index("zhi")
    core = lax.axis_index("core")
    for piece, zz, cc in (
        (z_same, 1 - zhi, core),
        (z_cross, 1 - zhi, 1 - core),
        (own, zhi, core),
        (swapped, zhi, 1 - core),
    ):
        left = pl.multiple_of((zz * 2 + cc) * HEAD, HEAD)
        out[:, pl.ds(left, HEAD)] = piece[...]


def along(value, axis, by):
    return lax.ppermute(value, axis, [(i, (i + by) % 4) for i in range(4)])


def mirror(value, axes):
    size = 2 if isinstance(axes, str) else 4
    return lax.ppermute(value, axes, [(i, size - 1 - i) for i in range(size)])


def layer(query, key, value, block_order):
    rows = query.shape[0]
    packed = pl.pallas_call(
        sort_kernel,
        out_shape=jax.ShapeDtypeStruct((16, rows, 4 * HEAD), jnp.bfloat16),
        in_specs=[pl.BlockSpec(memory_space=pltpu.HBM)] * 3,
        out_specs=pl.BlockSpec(memory_space=pltpu.HBM),
        scratch_shapes=[
            pltpu.VMEM(query.shape, jnp.bfloat16),
            pltpu.VMEM(key.shape, jnp.bfloat16),
            pltpu.VMEM(value.shape, jnp.bfloat16),
            pltpu.VMEM((16, rows, 4 * HEAD), jnp.bfloat16),
            pltpu.SemaphoreType.DMA((4,)),
        ],
        compiler_params=pltpu.CompilerParams(vmem_limit_bytes=62 * 1024 * 1024),
        name="k_sort",
    )(query, key, value)
    packed = lax.all_to_all(packed, ("y", "zlo", "zhi"), 0, 0)
    low, high, keep, send = local_call(
        split_kernel, [(8, rows, 2 * HEAD)] * 2 + [(16, rows, HEAD)] * 2, (packed,)
    )
    got = mirror(send, "core")
    up_low = along(low, "x", 1)
    down_high = along(high, "x", -1)
    up_high = along(high, "x", 1)
    down_low = along(low, "x", -1)
    far_low = along(up_low, "x", 1)
    far_high = along(down_high, "x", -1)

    def swap(half):
        return mirror(half, "core")

    own = [(low, 0, 0, 0), (high, 0, 0, 1)]
    own += [(swap(low), 0, 1, 0), (swap(high), 0, 1, 1)]
    near = [(up_low, 1, 0, 0), (down_high, 3, 0, 1)]
    near += [(swap(up_low), 1, 1, 0), (swap(down_high), 3, 1, 1)]
    rest = [(up_high, 1, 0, 1), (down_low, 3, 0, 0), (far_low, 2, 0, 0), (far_high, 2, 0, 1)]
    rest_o = [(swap(up_high), 1, 1, 1), (swap(down_low), 3, 1, 0)]
    rest_o += [(swap(far_low), 2, 1, 0), (swap(far_high), 2, 1, 1)]

    def step(given, halves, carry, first=False, last=False):
        return attend(block_order, given, halves, carry, first, last)

    both = (REMOTE, LOCAL)
    state = step(own, both, (keep, got), first=True)
    state = step(near, both, state)
    remote, local = state[:3], state[3:]
    remote = step(rest, (REMOTE,), remote)
    same, cross = step(rest_o, (REMOTE,), remote, last=True)
    z_same = mirror(same, "zhi")
    z_cross = mirror(cross, ("zhi", "core"))
    mine, cross = step(rest + rest_o, (LOCAL,), local, last=True)
    swapped = mirror(cross, "core")
    (out,) = local_call(assemble_kernel, [(2 * BLK, 4 * HEAD)], (mine, swapped, z_same, z_cross))
    return out


def solution(mesh):
    fine = Mesh(mesh.devices.reshape(4, 2, 2, 4, 2), AXES)
    placed = P(("zhi", "x", "core", "y", "zlo"), None)
    return jax.shard_map(
        layer,
        mesh=fine,
        in_specs=(placed, placed, placed, P()),
        out_specs=P(("zhi", "x", "core"), ("y", "zlo")),
        check_vma=False,
    )
```

```python
import functools

import jax
import jax.numpy as jnp
from jax import lax
from jax.experimental import pallas as pl
from jax.experimental.pallas import tpu as pltpu
from jax.sharding import Mesh
from jax.sharding import PartitionSpec as P

HEAD = 128
BLK = 384
PIECE = 96
TILE = 256
UNROLL = 4
SCORE_SCALE = 1.0 / (12.0 * 50.0)
CAP_LOG2E = 50.0 * 1.4426950408889634

AXES = ("y", "zlo", "zhi", "x", "core")
REMOTE, LOCAL, BOTH = 0, 1, 2
SLOTS = tuple((half, yhi, flip) for half in (REMOTE, LOCAL) for yhi in range(2) for flip in range(2))


def slots_of(half):
    return tuple(slot for slot in SLOTS if half in (slot[0], BOTH))


def attend_kernel(*refs, offsets, half, first, last, split):
    slots = slots_of(half)
    blocks = len(slots)
    tiles = blocks * BLK // TILE
    refs = list(refs)
    order = refs.pop(0)
    kv = [refs.pop(0) for _ in offsets]
    if first:
        q_refs = [refs.pop(0) for _ in range(2)]
    else:
        state_in = [refs.pop(0) for _ in range(3)]
    if last and half == REMOTE:
        both = refs.pop(0)
        outs = [both.at[0], both.at[1]]
    elif last:
        outs = [refs.pop(0) for _ in range(2)]
    else:
        states_out = [[refs.pop(0) for _ in range(3)] for _ in range(2 if split else 1)]
    qt, num, den, qpos, kbuf, vt = refs[:6]
    s_bufs = refs[6 : 6 + UNROLL]
    p_bufs = refs[6 + UNROLL : 6 + 2 * UNROLL]
    rows, q_seq, q_rank, kb_list, kb_start, kb_seq = refs[6 + 2 * UNROLL :]

    x = lax.axis_index("x")
    core = lax.axis_index("core")
    zhi = lax.axis_index("zhi")

    seqs = []
    for side, yhi, flip in slots:
        zz = 1 - zhi if side == REMOTE else zhi
        cc = 1 - core if flip else core
        seqs.append(order[2 * (zz * 8 + x * 2 + cc) + yhi])

    def rank_among(slot, others):
        rank = jnp.int32(0)
        for other in others:
            if other != slot:
                rank = rank + (seqs[other] < seqs[slot]).astype(jnp.int32)
        return rank

    for slot in range(blocks):
        rank = rank_among(slot, range(blocks))
        q_seq[rank] = seqs[slot]
        q_rank[slot] = rank
    lane = lax.broadcasted_iota(jnp.int32, (8, 128), 1)
    for g in range(2 * tiles):
        base = q_seq[g // 3] * BLK + (g % 3) * 128
        qpos[g // 2, :, (g % 2) * 128 : (g % 2) * 128 + 128] = lane + base
    qpos[tiles] = jnp.zeros((8, TILE), jnp.int32)

    if first:
        for slot, (side, yhi, flip) in enumerate(slots):
            zz = 1 - zhi if side == REMOTE else zhi
            top = pl.multiple_of(q_rank[slot] * BLK, BLK)
            for sub in range(4):
                piece = q_refs[flip][yhi * 8 + sub * 2 + zz]
                rows[pl.ds(top + sub * PIECE, PIECE), :] = piece
        for t in range(tiles):
            qt[t] = rows[t * TILE : (t + 1) * TILE, :].T
            num[t] = jnp.zeros((HEAD, TILE), jnp.float32)
            den[t] = jnp.zeros((8, TILE), jnp.float32)
    else:
        for t in range(tiles):
            qt[t] = state_in[0][t]
            num[t] = state_in[1][t]
            den[t] = state_in[2][t]
    qt[tiles] = jnp.zeros((HEAD, TILE), jnp.bfloat16)
    num[tiles] = jnp.zeros((HEAD, TILE), jnp.float32)
    den[tiles] = jnp.zeros((8, TILE), jnp.float32)

    count = jnp.int32(0)
    total = jnp.int32(0)
    for n, (dx, flip, yhi) in enumerate(offsets):
        xs = (x + (4 - dx)) % 4
        cs = 1 - core if flip else core
        for zz in range(2):
            kb = 2 * n + zz
            vals = []
            for sub in range(4):
                piece = kv[n][sub * 2 + zz]
                kbuf[kb, sub * PIECE : (sub + 1) * PIECE, :] = piece[:, :HEAD]
                vals.append(piece[:, HEAD:])
            vt[kb] = jnp.concatenate(vals, axis=0).T
            seq = order[2 * (zz * 8 + xs * 2 + cs) + yhi]
            below = jnp.int32(0)
            for slot in range(blocks):
                below = below + (seqs[slot] < seq).astype(jnp.int32)
            start = (3 * below) // 2
            kb_list[count] = jnp.int32(kb)
            kb_start[count] = start
            kb_seq[count] = seq
            count = count + (start < tiles).astype(jnp.int32)
            total = total + (tiles - start)
    for extra in range(2 * UNROLL + 2):
        kb_list[count + extra] = jnp.int32(0)
        kb_start[count + extra] = jnp.int32(tiles)
        kb_seq[count + extra] = jnp.int32(0)

    def after(item):
        j, t = item
        wrap = t + 1 >= tiles
        j = jnp.where(wrap, j + 1, j)
        return j, jnp.where(wrap, kb_start[j], t + 1)

    def score(item, s):
        j, t = item
        s[...] = jnp.dot(kbuf[kb_list[j]], qt[t], preferred_element_type=jnp.float32)

    row = lax.broadcasted_iota(jnp.int32, (8, TILE), 0)

    def weigh(item, s, p):
        j, t = item
        rel = qpos[t] - (kb_seq[j] * BLK + row)
        acc = None
        for r in range(0, BLK, 16):
            both = []
            for h in range(2):
                z = s[r + 8 * h : r + 8 * h + 8, :]
                w = jnp.exp2(CAP_LOG2E * jnp.tanh(z * SCORE_SCALE))
                w = jnp.where(rel >= r + 8 * h, w, 0.0)
                acc = w if acc is None else acc + w
                both.append(w)
            p[r : r + 16, :] = jnp.concatenate(both, axis=0).astype(jnp.bfloat16)
        den[t] = den[t] + acc

    def gather(item, p):
        j, t = item
        num[t] = num[t] + jnp.dot(vt[kb_list[j]], p[...], preferred_element_type=jnp.float32)

    items = [(jnp.int32(0), kb_start[0])]
    for _ in range(UNROLL - 1):
        items.append(after(items[-1]))
    for k in range(UNROLL):
        score(items[k], s_bufs[k])
    p_bufs[UNROLL - 1][...] = jnp.zeros((BLK, TILE), jnp.bfloat16)

    def body(_, state):
        cur, prev = state
        nxt = []
        item = cur[-1]
        for _ in range(UNROLL):
            item = after(item)
            nxt.append(item)
        weigh(cur[0], s_bufs[0], p_bufs[0])
        weigh(cur[1], s_bufs[1], p_bufs[1])
        gather(prev, p_bufs[3])
        score(nxt[0], s_bufs[0])
        score(nxt[1], s_bufs[1])
        gather(cur[0], p_bufs[0])
        weigh(cur[2], s_bufs[2], p_bufs[2])
        score(nxt[2], s_bufs[2])
        weigh(cur[3], s_bufs[3], p_bufs[3])
        gather(cur[1], p_bufs[1])
        gather(cur[2], p_bufs[2])
        score(nxt[3], s_bufs[3])
        return tuple(nxt), cur[-1]

    idle = (count, jnp.int32(tiles))
    _, tail = lax.fori_loop(0, (total + UNROLL - 1) // UNROLL, body, (tuple(items), idle))
    gather(tail, p_bufs[UNROLL - 1])

    if last:
        for t in range(tiles):
            inv = 1.0 / jnp.sum(den[t], axis=0, keepdims=True)
            rows[t * TILE : (t + 1) * TILE, :] = (num[t] * inv).T.astype(jnp.bfloat16)
        for slot, (_, yhi, flip) in enumerate(slots):
            top = pl.multiple_of(q_rank[slot] * BLK, BLK)
            outs[flip][yhi * BLK : (yhi + 1) * BLK, :] = rows[pl.ds(top, BLK), :]
    elif split:
        for slot in range(blocks):
            mates = range(0, 4) if slot < 4 else range(4, 8)
            to = rank_among(slot, mates) * 3
            at = q_rank[slot] * 3
            for j in range(3):
                source = pl.ds(pl.multiple_of(((at + j) % 2) * 128, 128), 128)
                target = pl.ds(pl.multiple_of(((to + j) % 2) * 128, 128), 128)
                for out, held in zip(states_out[slot // 4], (qt, num, den)):
                    out[(to + j) // 2, :, target] = held[(at + j) // 2, :, source]
    else:
        for t in range(tiles):
            for out, held in zip(states_out[0], (qt, num, den)):
                out[t] = held[t]


def attend(order, given, half, carry, first, last, split):
    kvs = [piece for piece, _, _, _ in given]
    offsets = tuple(at for _, *at in given)
    vmem = pl.BlockSpec(memory_space=pltpu.VMEM)
    smem = pl.BlockSpec(memory_space=pltpu.SMEM)
    nb = 2 * len(given)
    blocks = len(slots_of(half))
    tiles = blocks * BLK // TILE
    runs = nb + 2 * UNROLL + 4
    if last and half == REMOTE:
        out = (jax.ShapeDtypeStruct((2, 2 * BLK, HEAD), jnp.bfloat16),)
    elif last:
        out = (jax.ShapeDtypeStruct((2 * BLK, HEAD), jnp.bfloat16),) * 2
    else:
        kept = tiles // 2 if split else tiles
        out = (
            jax.ShapeDtypeStruct((kept, HEAD, TILE), jnp.bfloat16),
            jax.ShapeDtypeStruct((kept, HEAD, TILE), jnp.float32),
            jax.ShapeDtypeStruct((kept, 8, TILE), jnp.float32),
        ) * (2 if split else 1)
    inputs = [order, *kvs, *carry]
    return pl.pallas_call(
        functools.partial(
            attend_kernel, offsets=offsets, half=half, first=first, last=last, split=split
        ),
        out_shape=out,
        in_specs=[smem] + [vmem] * (len(inputs) - 1),
        out_specs=(vmem,) * len(out),
        scratch_shapes=[
            pltpu.VMEM((tiles + 1, HEAD, TILE), jnp.bfloat16),
            pltpu.VMEM((tiles + 1, HEAD, TILE), jnp.float32),
            pltpu.VMEM((tiles + 1, 8, TILE), jnp.float32),
            pltpu.VMEM((tiles + 1, 8, TILE), jnp.int32),
            pltpu.VMEM((nb, BLK, HEAD), jnp.bfloat16),
            pltpu.VMEM((nb, HEAD, BLK), jnp.bfloat16),
            *[pltpu.VMEM((BLK, TILE), jnp.float32) for _ in range(UNROLL)],
            *[pltpu.VMEM((BLK, TILE), jnp.bfloat16) for _ in range(UNROLL)],
            pltpu.VMEM((tiles * TILE, HEAD), jnp.bfloat16),
            pltpu.SMEM((blocks,), jnp.int32),
            pltpu.SMEM((blocks,), jnp.int32),
            pltpu.SMEM((runs,), jnp.int32),
            pltpu.SMEM((runs,), jnp.int32),
            pltpu.SMEM((runs,), jnp.int32),
        ],
        compiler_params=pltpu.CompilerParams(vmem_limit_bytes=28 * 1024 * 1024),
        cost_estimate=pl.CostEstimate(
            flops=len(given) * blocks * 150_000_000,
            transcendentals=0,
            bytes_accessed=4_000_000,
        ),
    )(*inputs)


def local_call(body, outs, inputs):
    vmem = pl.BlockSpec(memory_space=pltpu.VMEM)
    return pl.pallas_call(
        body,
        out_shape=tuple(jax.ShapeDtypeStruct(shape, jnp.bfloat16) for shape in outs),
        in_specs=[vmem] * len(inputs),
        out_specs=(vmem,) * len(outs),
        compiler_params=pltpu.CompilerParams(vmem_limit_bytes=8 * 1024 * 1024),
    )(*inputs)


def sort_kernel(query, key, value, out, q_rows, k_rows, v_rows, packed, sems):
    copies = [
        pltpu.make_async_copy(source, rows, sems.at[n])
        for n, (source, rows) in enumerate(((query, q_rows), (key, k_rows), (value, v_rows)))
    ]
    for copy in copies:
        copy.start()
    for copy in copies:
        copy.wait()
    for head in range(16):
        packed[head, :, : 2 * HEAD] = q_rows[:, 2 * head * HEAD : 2 * (head + 1) * HEAD]
        packed[head, :, 2 * HEAD : 3 * HEAD] = k_rows[:, head * HEAD : (head + 1) * HEAD]
        packed[head, :, 3 * HEAD :] = v_rows[:, head * HEAD : (head + 1) * HEAD]
    done = pltpu.make_async_copy(packed, out, sems.at[3])
    done.start()
    done.wait()


def split_kernel(got, low, high, keep, send):
    core = lax.axis_index("core")
    mine = pl.multiple_of(core * HEAD, HEAD)
    other = pl.multiple_of((1 - core) * HEAD, HEAD)
    for n in range(16):
        (low, high)[n // 8][n % 8] = got[n, :, 2 * HEAD :]
        keep[n] = got[n, :, pl.ds(mine, HEAD)]
        send[n] = got[n, :, pl.ds(other, HEAD)]


def assemble_kernel(own, swapped, across, across_o, out):
    zhi = lax.axis_index("zhi")
    core = lax.axis_index("core")
    for piece, zz, cc in (
        (across.at[0], 1 - zhi, core),
        (across_o.at[1], 1 - zhi, 1 - core),
        (own, zhi, core),
        (swapped, zhi, 1 - core),
    ):
        left = pl.multiple_of((zz * 2 + cc) * HEAD, HEAD)
        out[:, pl.ds(left, HEAD)] = piece[...]


def along(value, axis, by):
    return lax.ppermute(value, axis, [(i, (i + by) % 4) for i in range(4)])


def mirror(value, axes):
    size = 2 if isinstance(axes, str) else 4
    return lax.ppermute(value, axes, [(i, size - 1 - i) for i in range(size)])


def layer(query, key, value, block_order):
    rows = query.shape[0]
    packed = pl.pallas_call(
        sort_kernel,
        out_shape=jax.ShapeDtypeStruct((16, rows, 4 * HEAD), jnp.bfloat16),
        in_specs=[pl.BlockSpec(memory_space=pltpu.HBM)] * 3,
        out_specs=pl.BlockSpec(memory_space=pltpu.HBM),
        scratch_shapes=[
            pltpu.VMEM(query.shape, jnp.bfloat16),
            pltpu.VMEM(key.shape, jnp.bfloat16),
            pltpu.VMEM(value.shape, jnp.bfloat16),
            pltpu.VMEM((16, rows, 4 * HEAD), jnp.bfloat16),
            pltpu.SemaphoreType.DMA((4,)),
        ],
        compiler_params=pltpu.CompilerParams(vmem_limit_bytes=62 * 1024 * 1024),
        name="k_sort",
    )(query, key, value)
    packed = lax.all_to_all(packed, ("y", "zlo", "zhi"), 0, 0)
    low, high, keep, send = local_call(
        split_kernel, [(8, rows, 2 * HEAD)] * 2 + [(16, rows, HEAD)] * 2, (packed,)
    )
    got = mirror(send, "core")
    up_low = along(low, "x", 1)
    down_high = along(high, "x", -1)
    up_high = along(high, "x", 1)
    down_low = along(low, "x", -1)
    far_low = along(up_low, "x", 1)
    far_high = along(down_high, "x", -1)

    def swap(half):
        return mirror(half, "core")

    own = [(low, 0, 0, 0), (high, 0, 0, 1)]
    own += [(swap(low), 0, 1, 0), (swap(high), 0, 1, 1)]
    near = [(up_low, 1, 0, 0), (down_high, 3, 0, 1)]
    near += [(swap(up_low), 1, 1, 0), (swap(down_high), 3, 1, 1)]
    rest = [(up_high, 1, 0, 1), (down_low, 3, 0, 0), (far_low, 2, 0, 0), (far_high, 2, 0, 1)]
    rest_o = [(swap(up_high), 1, 1, 1), (swap(down_low), 3, 1, 0)]
    rest_o += [(swap(far_low), 2, 1, 0), (swap(far_high), 2, 1, 1)]

    def step(given, half, carry, first=False, last=False, split=False):
        return attend(block_order, given, half, carry, first, last, split)

    state = step(own, BOTH, (keep, got), first=True)
    state = step(near, BOTH, state, split=True)
    remote, local = state[:3], state[3:]
    remote = step(rest, REMOTE, remote)
    (sent,) = step(rest_o, REMOTE, remote, last=True)
    across = mirror(sent, "zhi")
    mine, cross = step(rest + rest_o, LOCAL, local, last=True)
    swapped = mirror(cross, "core")
    across_o = mirror(across, "core")
    (out,) = local_call(assemble_kernel, [(2 * BLK, 4 * HEAD)], (mine, swapped, across, across_o))
    return out


def solution(mesh):
    fine = Mesh(mesh.devices.reshape(4, 2, 2, 4, 2), AXES)
    placed = P(("zhi", "x", "core", "y", "zlo"), None)
    return jax.shard_map(
        layer,
        mesh=fine,
        in_specs=(placed, placed, placed, P()),
        out_specs=P(("zhi", "x", "core"), ("y", "zlo")),
        check_vma=False,
    )
```

```python
import functools

import jax
import jax.numpy as jnp
from jax import lax
from jax.experimental import pallas as pl
from jax.experimental.pallas import tpu as pltpu
from jax.sharding import Mesh
from jax.sharding import PartitionSpec as P

HEAD = 128
BLK = 384
PIECE = 96
TILE = 256
UNROLL = 4
SCORE_SCALE = 1.0 / (12.0 * 50.0)
CAP_LOG2E = 50.0 * 1.4426950408889634

AXES = ("y", "zlo", "zhi", "x", "core")
REMOTE, LOCAL, BOTH = 0, 1, 2
SLOTS = tuple((half, yhi, flip) for half in (REMOTE, LOCAL) for yhi in range(2) for flip in range(2))


def slots_of(half):
    return tuple(slot for slot in SLOTS if half in (slot[0], BOTH))


def attend_kernel(*refs, offsets, half, first, last, split):
    slots = slots_of(half)
    blocks = len(slots)
    tiles = blocks * BLK // TILE
    refs = list(refs)
    order = refs.pop(0)
    kv = [refs.pop(0) for _ in offsets]
    if first:
        q_refs = [refs.pop(0) for _ in range(2)]
    else:
        state_in = [refs.pop(0) for _ in range(3)]
    if last:
        outs = [refs.pop(0) for _ in range(2)]
    else:
        states_out = [[refs.pop(0) for _ in range(3)] for _ in range(2 if split else 1)]
    qt, num, den, qpos, kbuf, vt = refs[:6]
    s_bufs = refs[6 : 6 + UNROLL]
    p_bufs = refs[6 + UNROLL : 6 + 2 * UNROLL]
    rows, q_seq, q_rank, kb_list, kb_start, kb_seq = refs[6 + 2 * UNROLL :]

    x = lax.axis_index("x")
    core = lax.axis_index("core")
    zhi = lax.axis_index("zhi")

    seqs = []
    for side, yhi, flip in slots:
        zz = 1 - zhi if side == REMOTE else zhi
        cc = 1 - core if flip else core
        seqs.append(order[2 * (zz * 8 + x * 2 + cc) + yhi])

    def rank_among(slot, others):
        rank = jnp.int32(0)
        for other in others:
            if other != slot:
                rank = rank + (seqs[other] < seqs[slot]).astype(jnp.int32)
        return rank

    for slot in range(blocks):
        rank = rank_among(slot, range(blocks))
        q_seq[rank] = seqs[slot]
        q_rank[slot] = rank
    lane = lax.broadcasted_iota(jnp.int32, (8, 128), 1)
    for g in range(2 * tiles):
        base = q_seq[g // 3] * BLK + (g % 3) * 128
        qpos[g // 2, :, (g % 2) * 128 : (g % 2) * 128 + 128] = lane + base
    qpos[tiles] = jnp.zeros((8, TILE), jnp.int32)

    if first:
        for slot, (side, yhi, flip) in enumerate(slots):
            zz = 1 - zhi if side == REMOTE else zhi
            top = pl.multiple_of(q_rank[slot] * BLK, BLK)
            for sub in range(4):
                piece = q_refs[flip][yhi * 8 + sub * 2 + zz]
                rows[pl.ds(top + sub * PIECE, PIECE), :] = piece
        for t in range(tiles):
            qt[t] = rows[t * TILE : (t + 1) * TILE, :].T
            num[t] = jnp.zeros((HEAD, TILE), jnp.float32)
            den[t] = jnp.zeros((8, TILE), jnp.float32)
    else:
        for t in range(tiles):
            qt[t] = state_in[0][t]
            num[t] = state_in[1][t]
            den[t] = state_in[2][t]
    qt[tiles] = jnp.zeros((HEAD, TILE), jnp.bfloat16)
    num[tiles] = jnp.zeros((HEAD, TILE), jnp.float32)
    den[tiles] = jnp.zeros((8, TILE), jnp.float32)

    count = jnp.int32(0)
    total = jnp.int32(0)
    for n, (dx, flip, yhi) in enumerate(offsets):
        xs = (x + (4 - dx)) % 4
        cs = 1 - core if flip else core
        for zz in range(2):
            kb = 2 * n + zz
            vals = []
            for sub in range(4):
                piece = kv[n][sub * 2 + zz]
                kbuf[kb, sub * PIECE : (sub + 1) * PIECE, :] = piece[:, :HEAD]
                vals.append(piece[:, HEAD:])
            vt[kb] = jnp.concatenate(vals, axis=0).T
            seq = order[2 * (zz * 8 + xs * 2 + cs) + yhi]
            below = jnp.int32(0)
            for slot in range(blocks):
                below = below + (seqs[slot] < seq).astype(jnp.int32)
            start = (3 * below) // 2
            kb_list[count] = jnp.int32(kb)
            kb_start[count] = start
            kb_seq[count] = seq
            count = count + (start < tiles).astype(jnp.int32)
            total = total + (tiles - start)
    for extra in range(2 * UNROLL + 2):
        kb_list[count + extra] = jnp.int32(0)
        kb_start[count + extra] = jnp.int32(tiles)
        kb_seq[count + extra] = jnp.int32(0)

    def after(item):
        j, t = item
        wrap = t + 1 >= tiles
        j = jnp.where(wrap, j + 1, j)
        return j, jnp.where(wrap, kb_start[j], t + 1)

    def score(item, s):
        j, t = item
        s[...] = jnp.dot(kbuf[kb_list[j]], qt[t], preferred_element_type=jnp.float32)

    row = lax.broadcasted_iota(jnp.int32, (8, TILE), 0)

    def weigh(item, s, p):
        j, t = item
        rel = qpos[t] - (kb_seq[j] * BLK + row)
        acc = None
        for r in range(0, BLK, 16):
            both = []
            for h in range(2):
                z = s[r + 8 * h : r + 8 * h + 8, :]
                w = jnp.exp2(CAP_LOG2E * jnp.tanh(z * SCORE_SCALE))
                w = jnp.where(rel >= r + 8 * h, w, 0.0)
                acc = w if acc is None else acc + w
                both.append(w)
            p[r : r + 16, :] = jnp.concatenate(both, axis=0).astype(jnp.bfloat16)
        den[t] = den[t] + acc

    def gather(item, p):
        j, t = item
        num[t] = num[t] + jnp.dot(vt[kb_list[j]], p[...], preferred_element_type=jnp.float32)

    items = [(jnp.int32(0), kb_start[0])]
    for _ in range(UNROLL - 1):
        items.append(after(items[-1]))
    for k in range(UNROLL):
        score(items[k], s_bufs[k])
    p_bufs[UNROLL - 1][...] = jnp.zeros((BLK, TILE), jnp.bfloat16)

    def body(_, state):
        cur, prev = state
        nxt = []
        item = cur[-1]
        for _ in range(UNROLL):
            item = after(item)
            nxt.append(item)
        weigh(cur[0], s_bufs[0], p_bufs[0])
        weigh(cur[1], s_bufs[1], p_bufs[1])
        gather(prev, p_bufs[3])
        score(nxt[0], s_bufs[0])
        score(nxt[1], s_bufs[1])
        gather(cur[0], p_bufs[0])
        weigh(cur[2], s_bufs[2], p_bufs[2])
        score(nxt[2], s_bufs[2])
        weigh(cur[3], s_bufs[3], p_bufs[3])
        gather(cur[1], p_bufs[1])
        gather(cur[2], p_bufs[2])
        score(nxt[3], s_bufs[3])
        return tuple(nxt), cur[-1]

    idle = (count, jnp.int32(tiles))
    _, tail = lax.fori_loop(0, (total + UNROLL - 1) // UNROLL, body, (tuple(items), idle))
    gather(tail, p_bufs[UNROLL - 1])

    if last:
        for t in range(tiles):
            inv = 1.0 / jnp.sum(den[t], axis=0, keepdims=True)
            rows[t * TILE : (t + 1) * TILE, :] = (num[t] * inv).T.astype(jnp.bfloat16)
        for slot, (_, yhi, flip) in enumerate(slots):
            top = pl.multiple_of(q_rank[slot] * BLK, BLK)
            outs[flip][yhi * BLK : (yhi + 1) * BLK, :] = rows[pl.ds(top, BLK), :]
    elif split:
        for slot in range(blocks):
            mates = range(0, 4) if slot < 4 else range(4, 8)
            to = rank_among(slot, mates) * 3
            at = q_rank[slot] * 3
            for j in range(3):
                source = pl.ds(pl.multiple_of(((at + j) % 2) * 128, 128), 128)
                target = pl.ds(pl.multiple_of(((to + j) % 2) * 128, 128), 128)
                for out, held in zip(states_out[slot // 4], (qt, num, den)):
                    out[(to + j) // 2, :, target] = held[(at + j) // 2, :, source]
    else:
        for t in range(tiles):
            for out, held in zip(states_out[0], (qt, num, den)):
                out[t] = held[t]


def attend(order, given, half, carry, first, last, split):
    kvs = [piece for piece, _, _, _ in given]
    offsets = tuple(at for _, *at in given)
    vmem = pl.BlockSpec(memory_space=pltpu.VMEM)
    smem = pl.BlockSpec(memory_space=pltpu.SMEM)
    nb = 2 * len(given)
    blocks = len(slots_of(half))
    tiles = blocks * BLK // TILE
    runs = nb + 2 * UNROLL + 4
    if last:
        out = (jax.ShapeDtypeStruct((2 * BLK, HEAD), jnp.bfloat16),) * 2
    else:
        kept = tiles // 2 if split else tiles
        out = (
            jax.ShapeDtypeStruct((kept, HEAD, TILE), jnp.bfloat16),
            jax.ShapeDtypeStruct((kept, HEAD, TILE), jnp.float32),
            jax.ShapeDtypeStruct((kept, 8, TILE), jnp.float32),
        ) * (2 if split else 1)
    inputs = [order, *kvs, *carry]
    return pl.pallas_call(
        functools.partial(
            attend_kernel, offsets=offsets, half=half, first=first, last=last, split=split
        ),
        out_shape=out,
        in_specs=[smem] + [vmem] * (len(inputs) - 1),
        out_specs=(vmem,) * len(out),
        scratch_shapes=[
            pltpu.VMEM((tiles + 1, HEAD, TILE), jnp.bfloat16),
            pltpu.VMEM((tiles + 1, HEAD, TILE), jnp.float32),
            pltpu.VMEM((tiles + 1, 8, TILE), jnp.float32),
            pltpu.VMEM((tiles + 1, 8, TILE), jnp.int32),
            pltpu.VMEM((nb, BLK, HEAD), jnp.bfloat16),
            pltpu.VMEM((nb, HEAD, BLK), jnp.bfloat16),
            *[pltpu.VMEM((BLK, TILE), jnp.float32) for _ in range(UNROLL)],
            *[pltpu.VMEM((BLK, TILE), jnp.bfloat16) for _ in range(UNROLL)],
            pltpu.VMEM((tiles * TILE, HEAD), jnp.bfloat16),
            pltpu.SMEM((blocks,), jnp.int32),
            pltpu.SMEM((blocks,), jnp.int32),
            pltpu.SMEM((runs,), jnp.int32),
            pltpu.SMEM((runs,), jnp.int32),
            pltpu.SMEM((runs,), jnp.int32),
        ],
        compiler_params=pltpu.CompilerParams(vmem_limit_bytes=28 * 1024 * 1024),
        cost_estimate=pl.CostEstimate(
            flops=len(given) * blocks * 150_000_000,
            transcendentals=0,
            bytes_accessed=4_000_000,
        ),
    )(*inputs)


def local_call(body, outs, inputs):
    vmem = pl.BlockSpec(memory_space=pltpu.VMEM)
    return pl.pallas_call(
        body,
        out_shape=tuple(jax.ShapeDtypeStruct(shape, jnp.bfloat16) for shape in outs),
        in_specs=[vmem] * len(inputs),
        out_specs=(vmem,) * len(outs),
        compiler_params=pltpu.CompilerParams(vmem_limit_bytes=8 * 1024 * 1024),
    )(*inputs)


def sort_kernel(query, key, value, out, q_rows, k_rows, v_rows, packed, sems):
    copies = [
        pltpu.make_async_copy(source, rows, sems.at[n])
        for n, (source, rows) in enumerate(((query, q_rows), (key, k_rows), (value, v_rows)))
    ]
    for copy in copies:
        copy.start()
    for copy in copies:
        copy.wait()
    for head in range(16):
        packed[head, :, : 2 * HEAD] = q_rows[:, 2 * head * HEAD : 2 * (head + 1) * HEAD]
        packed[head, :, 2 * HEAD : 3 * HEAD] = k_rows[:, head * HEAD : (head + 1) * HEAD]
        packed[head, :, 3 * HEAD :] = v_rows[:, head * HEAD : (head + 1) * HEAD]
    done = pltpu.make_async_copy(packed, out, sems.at[3])
    done.start()
    done.wait()


def split_kernel(got, low, high, keep, send):
    core = lax.axis_index("core")
    mine = pl.multiple_of(core * HEAD, HEAD)
    other = pl.multiple_of((1 - core) * HEAD, HEAD)
    for n in range(16):
        (low, high)[n // 8][n % 8] = got[n, :, 2 * HEAD :]
        keep[n] = got[n, :, pl.ds(mine, HEAD)]
        send[n] = got[n, :, pl.ds(other, HEAD)]


def assemble_kernel(own, swapped, z_same, z_cross, out):
    zhi = lax.axis_index("zhi")
    core = lax.axis_index("core")
    for piece, zz, cc in (
        (z_same, 1 - zhi, core),
        (z_cross, 1 - zhi, 1 - core),
        (own, zhi, core),
        (swapped, zhi, 1 - core),
    ):
        left = pl.multiple_of((zz * 2 + cc) * HEAD, HEAD)
        out[:, pl.ds(left, HEAD)] = piece[...]


def along(value, axis, by):
    return lax.ppermute(value, axis, [(i, (i + by) % 4) for i in range(4)])


def mirror(value, axes):
    size = 2 if isinstance(axes, str) else 4
    return lax.ppermute(value, axes, [(i, size - 1 - i) for i in range(size)])


def layer(query, key, value, block_order):
    rows = query.shape[0]
    packed = pl.pallas_call(
        sort_kernel,
        out_shape=jax.ShapeDtypeStruct((16, rows, 4 * HEAD), jnp.bfloat16),
        in_specs=[pl.BlockSpec(memory_space=pltpu.HBM)] * 3,
        out_specs=pl.BlockSpec(memory_space=pltpu.HBM),
        scratch_shapes=[
            pltpu.VMEM(query.shape, jnp.bfloat16),
            pltpu.VMEM(key.shape, jnp.bfloat16),
            pltpu.VMEM(value.shape, jnp.bfloat16),
            pltpu.VMEM((16, rows, 4 * HEAD), jnp.bfloat16),
            pltpu.SemaphoreType.DMA((4,)),
        ],
        compiler_params=pltpu.CompilerParams(vmem_limit_bytes=62 * 1024 * 1024),
        name="k_sort",
    )(query, key, value)
    packed = lax.all_to_all(packed, ("y", "zlo", "zhi"), 0, 0)
    low, high, keep, send = local_call(
        split_kernel, [(8, rows, 2 * HEAD)] * 2 + [(16, rows, HEAD)] * 2, (packed,)
    )
    got = mirror(send, "core")
    up_low = along(low, "x", 1)
    down_high = along(high, "x", -1)
    up_high = along(high, "x", 1)
    down_low = along(low, "x", -1)
    far_low = along(up_low, "x", 1)
    far_high = along(down_high, "x", -1)

    def swap(half):
        return mirror(half, "core")

    own = [(low, 0, 0, 0), (high, 0, 0, 1)]
    own += [(swap(low), 0, 1, 0), (swap(high), 0, 1, 1)]
    near = [(up_low, 1, 0, 0), (down_high, 3, 0, 1)]
    near += [(swap(up_low), 1, 1, 0), (swap(down_high), 3, 1, 1)]
    rest = [(up_high, 1, 0, 1), (down_low, 3, 0, 0), (far_low, 2, 0, 0), (far_high, 2, 0, 1)]
    rest_o = [(swap(up_high), 1, 1, 1), (swap(down_low), 3, 1, 0)]
    rest_o += [(swap(far_low), 2, 1, 0), (swap(far_high), 2, 1, 1)]

    def step(given, half, carry, first=False, last=False, split=False):
        return attend(block_order, given, half, carry, first, last, split)

    state = step(own, BOTH, (keep, got), first=True)
    state = step(near, BOTH, state, split=True)
    remote, local = state[:3], state[3:]
    remote = step(rest, REMOTE, remote)
    same, cross = step(rest_o, REMOTE, remote, last=True)
    z_same = mirror(same, "zhi")
    z_cross = mirror(cross, ("zhi", "core"))
    mine, cross = step(rest + rest_o, LOCAL, local, last=True)
    swapped = mirror(cross, "core")
    (out,) = local_call(assemble_kernel, [(2 * BLK, 4 * HEAD)], (mine, swapped, z_same, z_cross))
    return out


def solution(mesh):
    fine = Mesh(mesh.devices.reshape(4, 2, 2, 4, 2), AXES)
    placed = P(("zhi", "x", "core", "y", "zlo"), None)
    return jax.shard_map(
        layer,
        mesh=fine,
        in_specs=(placed, placed, placed, P()),
        out_specs=P(("zhi", "x", "core"), ("y", "zlo")),
        check_vma=False,
    )
```
